256 devices in a mesh: dev: 128 (over z, y, x), rep: 2 (over core).
Axes of the slice: x: 4, y: 4, z: 8, core: 2. Of those that a mesh axis runs over, the one named last changes fastest.
Arguments:
- tables: bfloat16 [512, 2048, 128], P('dev'), may hold values from -1.5 to 1.5
- bag_rows: int32 [256, 512, 32, 4], P(('rep', 'dev')), parts along dimension 0, may hold values from 0 to 2047
- bag_lengths: int32 [256, 512, 32], P(('rep', 'dev')), parts along dimension 0, may hold values from 1 to 4
- row_counts: int32 [256, 512], P(('rep', 'dev')), parts along dimension 0, may hold values from 1 to 32, as said below
- inverse: int32 [32768, 512], P(('rep', 'dev')), parts along dimension 0, may hold values from 0 to 31
- table_order: int32 [512], replicated, may hold values from 0 to 511, each once
- compress: bfloat16 [16, 512], replicated, may hold values from -0.25 to 0.25
- top_weight: bfloat16 [8192, 512], replicated, may hold values from -0.0625 to 0.0625
- top_bias: float32 [512], replicated, may hold values from -1.8 to 1.8
Outputs:
- ranked: bfloat16 [32768, 512], P(('rep', 'dev')), parts along dimension 0
The draws below stay inside these ranges and needn't reach their ends.
There are 2 independent parts, one for each index of `rep`. The reference program is written for one: setup_inputs(seed, part) draws one part's arguments, and reference() takes and returns one part's arrays. A program takes and returns all parts, laid end to end along the dimension named above; an argument that names none is the same for every part. Nothing has to cross between parts.
Inputs may be any that keep to these rules, and one draw needn't show every extreme that they name: `row_counts`: for every sample device and every aligned group of 4 consecutive slots the counts sum to at most 80; a count of 32 and a group sum of 80 occur in every draw.
All inputs are finite; a program needn't handle non-finite values.
Results may differ from the reference program's by a relative error of at most 0.0062.
Values may be sent and summed in bfloat16 or wider, within the bound.
A program may use at most 128 MiB of HBM per device.

```python
import math
import jax
import jax.numpy as jnp
import numpy as np
from jax import lax

WIDTH = 128
VOCABULARY = 2048
TABLES_DEV = 4
TABLES = 512
BATCH_DEV = 128
BATCH = 16384
ROWS_MOST = 32
PACK_ROOM = 80
POOLING = 4
COMPRESSED = 16
TOP_UNITS = 512
N_DEV = 128


def draw_row_counts(key, part):
    first_key = jax.random.fold_in(key, 11)
    second_key = jax.random.fold_in(key, 12)
    third_key = jax.random.fold_in(key, 13)
    raw_counts = jax.random.randint(first_key, (N_DEV, N_DEV, TABLES_DEV), 1, ROWS_MOST + 1)
    group_total = jnp.sum(raw_counts, axis=2, keepdims=True)
    shrunk = 1 + (raw_counts - 1) * (PACK_ROOM - TABLES_DEV) // jnp.maximum(group_total - TABLES_DEV, 1)
    scaled = jnp.where(group_total > PACK_ROOM, shrunk, raw_counts)
    shift_value = jax.random.randint(second_key, (), 0, 5)
    device_range = jnp.arange(N_DEV, dtype=jnp.int32)[:, None]
    group_range = jnp.arange(N_DEV, dtype=jnp.int32)[None, :]
    forced = (device_range * 3 + group_range + shift_value) % 5 == 0
    leader = jax.random.randint(third_key, (N_DEV, N_DEV), 0, TABLES_DEV)
    remainder = PACK_ROOM - ROWS_MOST
    share_value = remainder // (TABLES_DEV - 1)
    last_value = remainder - (TABLES_DEV - 2) * share_value
    member = jnp.arange(TABLES_DEV, dtype=jnp.int32)[None, None, :]
    ranking = (member - leader[..., None]) % TABLES_DEV
    filled = jnp.where(ranking == 0, ROWS_MOST, jnp.where(ranking == TABLES_DEV - 1, last_value, share_value))
    result = jnp.where(forced[..., None], filled, scaled)
    return result.reshape(N_DEV, TABLES).astype(jnp.int32)


def with_ends(values, rng, smallest, largest):
    longest = values.shape.index(max(values.shape))
    spots = []
    for shift in (0, 1):
        where = [jax.random.randint(jax.random.fold_in(rng, axis), (), 0, length) for axis, length in enumerate(values.shape)]
        where[longest] = (where[longest] + shift) % values.shape[longest]
        spots.append(tuple(where))
    return values.at[spots[0]].set(smallest).at[spots[1]].set(largest)


def levels(own_key, dims, cuts, least, top_value):
    factor_of, own = 1.0, jax.random.fold_in(own_key, 6)
    for axis_at, blocks in cuts:
        heights = jnp.exp(jax.random.uniform(jax.random.fold_in(own, axis_at), (blocks,), jnp.float32, least / len(cuts), top_value / len(cuts)))
        factor_of = factor_of * jnp.repeat(heights, dims[axis_at] // blocks).reshape([-1 if axis == axis_at else 1 for axis in range(len(dims))])
    return factor_of


def rank_bounds(count, skew):
    weights = [(1 << 20) // math.isqrt(standing ** skew) + 1 for standing in range(1, count + 1)]
    width = 1 + sum(weights) // (1 << 30)
    return np.cumsum(np.array([max(1, weight // width) for weight in weights]))


def ranked_ids(stream_key, extent, number_of, skew):
    listing = rank_bounds(number_of, skew)
    pick = jax.random.randint(jax.random.fold_in(stream_key, 1), extent, 0, int(listing[number_of - 1]))
    rank = jnp.searchsorted(jnp.asarray(listing, jnp.int32), pick, side="right")
    return jax.random.permutation(jax.random.fold_in(stream_key, 2), number_of)[rank].astype(jnp.int32)


def gaussian(own_key, dims, scale, bound, split=(), kind=jnp.bfloat16):
    drawn = scale * jax.random.normal(own_key, dims, jnp.float32)
    if split:
        drawn = drawn * levels(own_key, dims, split, -0.22, 0.18)
    return jnp.clip(drawn, -bound, bound).astype(kind)


def setup_inputs(seed: int = 0, part: int = 0) -> dict:
    seeds = jax.random.split(jax.random.key(seed), 10)
    part_keys = jax.random.split(jax.random.fold_in(seeds[9], part), 10)
    tables = gaussian(seeds[0], (TABLES, VOCABULARY, WIDTH), 0.25, 1.5, ((0, 128),))
    bag_rows = with_ends(ranked_ids(part_keys[1], (N_DEV, TABLES, ROWS_MOST, POOLING), VOCABULARY, 2), jax.random.fold_in(part_keys[1], 3), 0, VOCABULARY - 1).astype(jnp.int32)
    bag_lengths = with_ends(jax.random.randint(part_keys[2], (N_DEV, TABLES, ROWS_MOST), 1, POOLING + 1), jax.random.fold_in(part_keys[2], 1), 1, POOLING).astype(jnp.int32)
    row_counts = draw_row_counts(jax.random.fold_in(jax.random.fold_in(seeds[9], part), 71), part)
    inverse = with_ends(jax.random.randint(part_keys[4], (BATCH, TABLES), 0, ROWS_MOST), jax.random.fold_in(part_keys[4], 1), 0, ROWS_MOST - 1).astype(jnp.int32)
    table_order = jax.random.permutation(seeds[5], TABLES).astype(jnp.int32)
    compress = gaussian(seeds[6], (COMPRESSED, TABLES), TABLES ** -0.5, 0.25)
    top_weight = gaussian(seeds[7], (TABLES * COMPRESSED, TOP_UNITS), (TABLES * COMPRESSED) ** -0.5, 0.0625)
    top_bias = gaussian(seeds[8], (TOP_UNITS,), 0.3, 1.8, (), jnp.float32)
    return {"tables": tables, "bag_rows": bag_rows, "bag_lengths": bag_lengths, "row_counts": row_counts, "inverse": inverse, "table_order": table_order, "compress": compress, "top_weight": top_weight, "top_bias": top_bias}


def pool_rows(tables, rows_here, lengths_here):
    gathered = jax.vmap(lambda one_table, one_bag: jnp.take(one_table, one_bag, axis=0))(tables, rows_here)
    active = jnp.arange(rows_here.shape[2], dtype=jnp.int32)[None, None, :] < lengths_here[..., None]
    summed = jnp.sum(jnp.where(active[..., None], gathered.astype(jnp.float32), jnp.zeros((), jnp.float32)), axis=2)
    return summed.astype(jnp.bfloat16)


def interact(features, compress, top_weight, top_bias):
    mixed = jnp.einsum("kf,bfe->bke", compress.astype(jnp.float32), features.astype(jnp.float32)).astype(jnp.bfloat16)
    pairwise = jnp.einsum("bfe,bke->bfk", features.astype(jnp.float32), mixed.astype(jnp.float32)).astype(jnp.bfloat16)
    hidden_pre = jnp.dot(pairwise.reshape(pairwise.shape[0], -1), top_weight, preferred_element_type=jnp.float32) + top_bias
    return jnp.maximum(hidden_pre, jnp.zeros((), jnp.float32)).astype(jnp.bfloat16)


def reference(tables, bag_rows, bag_lengths, row_counts, inverse, table_order, compress, top_weight, top_bias):
    slot_range = jnp.arange(TABLES, dtype=jnp.int32)
    matches = table_order[:, None] == slot_range[None, :]
    slot_of = jnp.sum(jnp.where(matches, slot_range[:, None], 0), axis=0).astype(jnp.int32)

    def one_device(device):
        rows_here = lax.dynamic_index_in_dim(bag_rows, device, 0, keepdims=False)
        lengths_here = lax.dynamic_index_in_dim(bag_lengths, device, 0, keepdims=False)
        counts_here = lax.dynamic_index_in_dim(row_counts, device, 0, keepdims=False)
        inverse_here = lax.dynamic_slice_in_dim(inverse, (device * BATCH_DEV).astype(jnp.int32), BATCH_DEV, 0)
        pooled = pool_rows(tables, rows_here, lengths_here)
        flat_rows = pooled.reshape(-1, WIDTH)
        positions = (slot_of[None, :] * ROWS_MOST + inverse_here).astype(jnp.int32)
        gathered = jnp.take(flat_rows, positions, axis=0)
        present = inverse_here < counts_here[slot_of][None, :]
        features = jnp.where(present[..., None], gathered, jnp.zeros((), jnp.bfloat16))
        return interact(features, compress, top_weight, top_bias)

    result = lax.map(one_device, jnp.arange(N_DEV, dtype=jnp.int32))
    return result.reshape(BATCH, TOP_UNITS)
```

```python
import functools
import jax
import jax.numpy as jnp
from jax import lax
from jax.experimental import pallas as pl
from jax.experimental.pallas import tpu as pltpu
from jax.sharding import PartitionSpec as P

BF = jnp.bfloat16
F32 = jnp.float32
I32 = jnp.int32
ROOM = 80


def iota(shape, axis):
    return lax.broadcasted_iota(I32, shape, axis)


def onehot(mask):
    return jnp.where(mask, 1.0, 0.0).astype(BF)


def prep_body(rows_ref, lens_ref, counts_ref, out_ref):
    most, pool, slots = rows_ref.shape
    used = iota((most, slots), 0) < counts_ref[...]
    lens = lens_ref[...]
    parts = [
        jnp.where(used & (p < lens), rows_ref[:, p, :], -1) for p in range(pool)
    ]
    wide = jnp.concatenate(parts, axis=0)
    for at in range(slots // 128):
        out_ref[pl.ds(at * 128, 128), :] = wide[:, at * 128 : (at + 1) * 128].T


def pool_setup(tables_ref, ids_ref, turned_ref, y_ref, pos_ref):
    tabs, vocab, width = tables_ref.shape
    for j in range(tabs):
        for at in range(vocab // 128):
            turned_ref[j, :, pl.ds(at * 128, 128)] = tables_ref[
                j, pl.ds(at * 128, 128), :
            ].astype(F32).T.astype(BF)
    lane = iota((32, 128), 1)
    chunk = lane // 32
    same = onehot(iota((128, 128), 0) // 32 == iota((128, 128), 1) // 32)
    base = jnp.zeros((32, 128), F32)
    for j in range(4):
        got = [ids_ref[pl.ds(4 * q + j, 32, stride=16), :] for q in range(4)]
        for p in range(4):
            y = got[0] if p == 0 else pltpu.roll(got[0], (-p * 32) % 128, 1)
            for q in range(1, 4):
                moved = got[q] if p == q else pltpu.roll(got[q], ((q - p) * 32) % 128, 1)
                y = jnp.where(chunk == q, moved, y)
            y_ref[pl.ds((j * 4 + p) * 32, 32), :] = y
            if p == 0:
                valid = y >= 0
                total = jnp.dot(onehot(valid), same, preferred_element_type=F32)
                place = base.astype(I32) + (lane % 32) + chunk * ROOM
                pos_ref[pl.ds(j * 32, 32), :] = jnp.where(valid, place, -1)
                base = base + total


def pool_pair(t, turned_ref, y_ref, pos_ref, hot_ref, xt_ref):
    width = turned_ref.shape[1]
    low_iota = iota((128, 128), 0)

    def table(j, carry):
        for half in range(2):
            lows, highs = [], []
            for p in range(4):
                y = y_ref[pl.ds((j * 4 + p) * 32 + 2 * t + half, 1), :]
                lows.append(onehot(jnp.broadcast_to(y & 127, (128, 128)) == low_iota))
                highs.append(jnp.broadcast_to(y >> 7, (16, 128)))
            for h in range(16):
                pick = [onehot(high == h) for high in highs]
                for at in range(8):
                    cut = [low[at * 16 : at * 16 + 16, :] for low in lows]
                    hot_ref[
                        pl.ds(h * 128 + at * 16, 16), half * 128 : half * 128 + 128
                    ] = (cut[0] * pick[0] + cut[1] * pick[1]) + (
                        cut[2] * pick[2] + cut[3] * pick[3]
                    )
        pooled = jnp.dot(
            turned_ref[j], hot_ref[...], preferred_element_type=F32
        ).astype(BF)
        xt_ref[0, j] = pooled[:, :128]
        xt_ref[1, j] = pooled[:, 128:]
        return carry

    lax.fori_loop(0, 4, table, 0)
    out = []
    for half in range(2):
        total = None
        for jj in range(2):
            packs, cols = [], []
            for j in (2 * jj, 2 * jj + 1):
                pos = pos_ref[pl.ds(j * 32 + 2 * t + half, 1), :]
                packs.append(
                    onehot(
                        jnp.broadcast_to(pos, (4 * ROOM, 128)) == iota((4 * ROOM, 128), 0)
                    )
                )
                cols.append(xt_ref[half, j])
            part = lax.dot_general(
                jnp.concatenate(packs, axis=1),
                jnp.concatenate(cols, axis=1),
                (((1,), (1,)), ((), ())),
                preferred_element_type=F32,
            )
            total = part if total is None else total + part
        out.append(total.astype(BF))
    return out


def pool_body(tables_ref, ids_ref, out_ref, turned_ref, y_ref, pos_ref, hot_ref, xt_ref):
    pool_setup(tables_ref, ids_ref, turned_ref, y_ref, pos_ref)

    def step(t, carry):
        blocks = pool_pair(t, turned_ref, y_ref, pos_ref, hot_ref, xt_ref)
        for half in range(2):
            out_ref[pl.ds(pl.multiple_of((2 * t + half) * 4 * ROOM, 4 * ROOM), 4 * ROOM), :] = blocks[half]
        return carry

    lax.fori_loop(0, 16, step, 0)


def pool_scratch():
    return [
        pltpu.VMEM((4, 128, 2048), BF),
        pltpu.VMEM((512, 128), I32),
        pltpu.VMEM((128, 128), I32),
        pltpu.VMEM((2048, 256), BF),
        pltpu.VMEM((2, 4, 128, 128), BF),
    ]


def order_columns(order_ref):
    slots = order_ref.shape[1]
    return onehot(iota((slots, slots), 0) == order_ref[...])


def weight_body(order_ref, top_ref, out_ref, plane_ref):
    slots, units = out_ref.shape[1:]
    row = iota((256, 256), 0)
    col = iota((256, 256), 1)
    spread = onehot((col % 16 == row // 16) & (col // 16 == row % 16))

    def cut(at, carry):
        block = jnp.dot(
            spread, top_ref[pl.ds(pl.multiple_of(at * 256, 256), 256), :], preferred_element_type=F32
        ).astype(BF)
        for k in range(16):
            plane_ref[k, pl.ds(pl.multiple_of(at * 16, 16), 16), :] = block[k * 16 : k * 16 + 16, :]
        return carry

    lax.fori_loop(0, slots // 16, cut, 0)
    perm = order_columns(order_ref).astype(F32).T.astype(BF)

    def turn(k, carry):
        out_ref[k] = jnp.dot(perm, plane_ref[k], preferred_element_type=F32).astype(BF)
        return carry

    lax.fori_loop(0, 16, turn, 0)


def target_setup(inverse_ref, counts_ref, order_ref, compress_ref, turn_ref, mix_ref):
    samples, slots = inverse_ref.shape
    columns = order_columns(order_ref)
    mix_ref[...] = jnp.dot(compress_ref[...], columns, preferred_element_type=F32).astype(BF)
    chosen = jnp.dot(inverse_ref[...].astype(F32).astype(BF), columns, preferred_element_type=F32)
    counts = jnp.broadcast_to(counts_ref[...], (16, slots)).astype(F32)
    before = (iota((slots, slots), 0) // 4 == iota((slots, slots), 1) // 4) & (
        iota((slots, slots), 0) < iota((slots, slots), 1)
    )
    base = jnp.dot(counts.astype(BF), onehot(before), preferred_element_type=F32)[:1, :]
    offset = ((iota((1, slots), 1) // 4) % 2 * ROOM).astype(F32)
    place = jnp.where(chosen < counts[:1, :], chosen + (base + offset), -1.0)
    for at in range(slots // 128):
        turn_ref[pl.ds(at * 128, 128), :] = place[:, at * 128 : (at + 1) * 128].T


def pick_half(slot, rows, turn_ref, lhs_ref):
    place = turn_ref[pl.ds(pl.multiple_of(slot, 8), 8), :]
    lanes = iota((8, 128), 1).astype(F32)
    for b in range(0, 128, 2):
        left = [jnp.broadcast_to(place[:, b + i : b + i + 1], (8, 128)) for i in range(2)]
        near = jnp.concatenate([jnp.where(x == lanes, 1.0, 0.0) for x in left], axis=0)
        far = jnp.concatenate([jnp.where(x == lanes + 128.0, 1.0, 0.0) for x in left], axis=0)
        lhs_ref[b * 8 : b * 8 + 16, 0:128] = near.astype(BF)
        lhs_ref[b * 8 : b * 8 + 16, 128:256] = far.astype(BF)
    return jnp.dot(lhs_ref[:, :160], rows, preferred_element_type=F32)


def pick_chunk(c, packed_ref, turn_ref, lhs_ref, feat_ref):
    halves = []
    for half in range(2):
        rows = packed_ref[pl.ds(pl.multiple_of(c * 320 + half * 160, 160), 160), :]
        halves.append(pick_half(c * 16 + half * 8, rows, turn_ref, lhs_ref).reshape(128, 8, 128))
    both = jnp.concatenate(halves, axis=1).astype(BF).reshape(64, 2, 16, 128)
    at = pl.ds(pl.multiple_of(c * 16, 16), 16)
    feat_ref[:, at, 0:128] = both[:, 0]
    feat_ref[:, at, 128:256] = both[:, 1]


def finish(feat_ref, mix_ref, weight_ref, bias_ref, out_ref, pair_ref, acc_ref):
    mix = mix_ref[...]
    zero = jnp.zeros((16, 128), BF)

    def pair(i, carry):
        feats = feat_ref[i]
        mixed = jnp.dot(mix, feats, preferred_element_type=F32).astype(BF)
        lhs = jnp.concatenate(
            [
                jnp.concatenate([mixed[:, :128], zero], axis=1),
                jnp.concatenate([zero, mixed[:, 128:]], axis=1),
            ],
            axis=0,
        )
        both = lax.dot_general(
            lhs, feats, (((1,), (1,)), ((), ())), preferred_element_type=F32
        )
        for at in range(4):
            pair_ref[at, pl.ds(pl.multiple_of(i * 32, 32), 32), :] = both[:, at * 128 : at * 128 + 128]
        return carry

    lax.fori_loop(0, feat_ref.shape[0], pair, 0)
    acc_ref[...] = jnp.broadcast_to(bias_ref[...], acc_ref.shape)

    def plane(k, carry):
        lhs = jnp.concatenate(
            [pair_ref[at, pl.ds(k, 128, stride=16), :].astype(BF) for at in range(4)], axis=1
        )
        acc_ref[...] += jnp.dot(lhs, weight_ref[k], preferred_element_type=F32)
        return carry

    lax.fori_loop(0, 16, plane, 0)
    out_ref[...] = jnp.maximum(acc_ref[...], 0.0).astype(BF)


def score_body(
    packed_ref, inverse_ref, counts_ref, order_ref, compress_ref, weight_ref, bias_ref,
    out_ref, turn_ref, mix_ref, lhs_ref, feat_ref, pair_ref, acc_ref,
):
    target_setup(inverse_ref, counts_ref, order_ref, compress_ref, turn_ref, mix_ref)

    def chunk(c, carry):
        pick_chunk(c, packed_ref, turn_ref, lhs_ref, feat_ref)
        return carry

    lax.fori_loop(0, 32, chunk, 0)
    finish(feat_ref, mix_ref, weight_ref, bias_ref, out_ref, pair_ref, acc_ref)


def score_scratch():
    return [
        pltpu.VMEM((512, 128), F32),
        pltpu.VMEM((16, 512), BF),
        pltpu.VMEM((1024, 256), BF),
        pltpu.VMEM((64, 512, 256), BF),
        pltpu.VMEM((4, 2048, 128), F32),
        pltpu.VMEM((128, 512), F32),
    ]


VM = pl.BlockSpec(memory_space=pltpu.VMEM)
BIG = 60 * 1024 * 1024


def call(body, outs, scratch, count, flops, **kw):
    return pl.pallas_call(
        body,
        out_shape=outs,
        in_specs=[VM] * count,
        out_specs=VM,
        scratch_shapes=scratch,
        compiler_params=pltpu.CompilerParams(vmem_limit_bytes=BIG, **kw),
        cost_estimate=pl.CostEstimate(flops=flops, bytes_accessed=4 << 20, transcendentals=0),
    )


def shards(tables, bag_rows, bag_lengths, row_counts, inverse, table_order, compress, top_weight, top_bias):
    order = table_order.reshape(1, -1)
    bias = top_bias.reshape(1, -1)
    slots = table_order.shape[0]
    rows = bag_rows[0].transpose(1, 2, 0)
    lens = bag_lengths[0].transpose(1, 0)
    ids = call(prep_body, jax.ShapeDtypeStruct((slots, 128), I32), [], 3, 10**6)(rows, lens, row_counts)
    got = lax.all_to_all(ids.reshape(128, 4, 128), "dev", split_axis=0, concat_axis=0, tiled=True)
    packed = call(pool_body, jax.ShapeDtypeStruct((128 * ROOM, 128), BF), pool_scratch(), 2, 9 * 10**9)(
        tables, got.reshape(512, 128)
    )
    arrived = lax.all_to_all(packed.reshape(128, ROOM, 128), "dev", split_axis=0, concat_axis=0, tiled=True)
    weight = call(
        weight_body,
        jax.ShapeDtypeStruct((16, slots, 512), BF),
        [pltpu.VMEM((16, slots, 512), BF)],
        2,
        6 * 10**9,
    )(order, top_weight)
    return call(score_body, jax.ShapeDtypeStruct((128, 512), BF), score_scratch(), 7, 10**10)(
        arrived.reshape(128 * ROOM, 128), inverse, row_counts, order, compress, weight, bias
    )


def solution(mesh):
    return jax.shard_map(
        shards,
        mesh=mesh,
        in_specs=(
            P("dev", None, None),
            P(("rep", "dev"), None, None, None),
            P(("rep", "dev"), None, None),
            P(("rep", "dev"), None),
            P(("rep", "dev"), None),
            P(),
            P(),
            P(),
            P(),
        ),
        out_specs=P(("rep", "dev"), None),
        check_vma=False,
    )
```

```python
import functools
import jax
import jax.numpy as jnp
from jax import lax
from jax.experimental import pallas as pl
from jax.experimental.pallas import tpu as pltpu
from jax.sharding import PartitionSpec as P

BF = jnp.bfloat16
F32 = jnp.float32
I32 = jnp.int32
ROOM = 80


def iota(shape, axis):
    return lax.broadcasted_iota(I32, shape, axis)


def onehot(mask):
    return jnp.where(mask, 1.0, 0.0).astype(BF)


def prep_body(rows_ref, lens_ref, counts_ref, out_ref):
    most, pool, slots = rows_ref.shape
    used = iota((most, slots), 0) < counts_ref[...]
    lens = lens_ref[...]
    parts = [
        jnp.where(used & (p < lens), rows_ref[:, p, :], -1) for p in range(pool)
    ]
    wide = jnp.concatenate(parts, axis=0)
    for at in range(slots // 128):
        out_ref[pl.ds(at * 128, 128), :] = wide[:, at * 128 : (at + 1) * 128].T


def prep_ids(rows_ref, lens_ref, counts_ref, ids_out):
    most, pool, slots = rows_ref.shape
    used = iota((most, slots), 0) < counts_ref[...]
    lens = lens_ref[...]
    wide = jnp.concatenate(
        [jnp.where(used & (p < lens), rows_ref[:, p, :], -1) for p in range(pool)], axis=0
    )
    for at in range(slots // 128):
        turned = wide[:, at * 128 : (at + 1) * 128].T.reshape(32, 4, 128)
        ids_out[at * 32 : at * 32 + 32] = turned.astype(jnp.int16)


PLANE = 512


def pool_turn(tables_ref, turned_ref):
    tabs, vocab, width = tables_ref.shape
    for j in range(tabs):
        for at in range(vocab // 128):
            turned_ref[j, at] = (
                tables_ref[j, at * 128 : at * 128 + 128, :].astype(F32).T * (0.25 ** (at % 4))
            ).astype(BF)


def pool_setup(load_ids, y_ref, code_ref, pos_ref, scale_ref):
    lane = iota((32, 128), 1)
    chunk = lane // 32
    same = onehot(iota((128, 128), 0) // 32 == iota((128, 128), 1) // 32)
    base = jnp.zeros((32, 128), F32)
    for j in range(4):
        got = [load_ids(q, j) for q in range(4)]
        ys = []
        for p in range(4):
            y = got[0] if p == 0 else pltpu.roll(got[0], (-p * 32) % 128, 1)
            for q in range(1, 4):
                moved = got[q] if p == q else pltpu.roll(got[q], ((q - p) * 32) % 128, 1)
                y = jnp.where(chunk == q, moved, y)
            ys.append(y)
        valid = ys[0] >= 0
        total = jnp.dot(onehot(valid), same, preferred_element_type=F32)
        place = base.astype(I32) + (lane % 32) + chunk * ROOM
        pos_ref[pl.ds(j * 32, 32), :] = jnp.where(valid, place, -1)
        base = base + total
        alike = (ys[0] == ys[1]) & (ys[0] == ys[2]) & (ys[0] == ys[3])
        scale_ref[pl.ds(j * 32, 32), :] = jnp.where(alike, 2.0, 1.0)
        for p in range(4):
            y = ys[p]
            live = (y >= 0) if p < 2 else ((y >= 0) & ~alike)
            code = jnp.where(live, jnp.left_shift(jnp.ones_like(y), ((y >> 7) * 2) & 31), 0)
            y_ref[pl.ds((j * 4 + p) * 32, 32), :] = y & 127
            for k in range(4):
                code_ref[pl.ds(k * PLANE + (j * 4 + p) * 32, 32), :] = (
                    lax.shift_right_logical(code, jnp.full_like(code, 8 * k)) & 255
                )


def small(ref, at):
    return jnp.broadcast_to(ref[pl.ds(at, 1), :], (16, 128)).astype(jnp.int16)


def pool_table(t, j, turned_ref, y_ref, code_ref, scale_ref, xt_ref):
    low_iota = iota((16, 128), 0).astype(jnp.int16)
    zero = jnp.zeros((16, 128), jnp.int16)
    rows = [[(j * 4 + p) * 32 + 2 * t + half for p in range(4)] for half in range(2)]
    hits = []
    for half in range(2):
        lows = [small(y_ref, row) for row in rows[half]]
        hits.append([[low == low_iota + jnp.int16(16 * at) for low in lows] for at in range(8)])
    total = None
    for k in range(4):
        planes = []
        for half in range(2):
            codes = [small(code_ref, k * PLANE + row) for row in rows[half]]
            plane = []
            for hit in hits[half]:
                cut = [jnp.where(hit[p], codes[p], zero) for p in range(4)]
                plane.append((cut[0] + cut[1]) + (cut[2] + cut[3]))
            planes.append(jnp.concatenate(plane, axis=0).astype(jnp.uint8))
        for i in (0, 2):
            hot = jnp.concatenate(
                [
                    jnp.concatenate([(plane & jnp.uint8(3 << (2 * u))).astype(BF) for u in (i, i + 1)], axis=0)
                    for plane in planes
                ],
                axis=1,
            )
            left = jnp.concatenate([turned_ref[j, 4 * k + i], turned_ref[j, 4 * k + i + 1]], axis=1)
            part = jnp.dot(left, hot, preferred_element_type=F32)
            total = part if total is None else total + part
    for half in range(2):
        scale = scale_ref[pl.ds(j * 32 + 2 * t + half, 1), :]
        xt_ref[half, j] = (total[:, half * 128 : half * 128 + 128] * scale).astype(BF)


def pool_pack(t, pos_ref, xt_ref):
    out = []
    for half in range(2):
        total = None
        for jj in range(2):
            packs, cols = [], []
            for j in (2 * jj, 2 * jj + 1):
                pos = small(pos_ref, j * 32 + 2 * t + half)
                hits = [
                    jnp.where(
                        pos == iota((16, 128), 0).astype(jnp.int16) + jnp.int16(16 * at),
                        jnp.ones((16, 128), BF),
                        jnp.zeros((16, 128), BF),
                    )
                    for at in range(4 * ROOM // 16)
                ]
                packs.append(jnp.concatenate(hits, axis=0))
                cols.append(xt_ref[half, j])
            part = lax.dot_general(
                jnp.concatenate(packs, axis=1),
                jnp.concatenate(cols, axis=1),
                (((1,), (1,)), ((), ())),
                preferred_element_type=F32,
            )
            total = part if total is None else total + part
        out.append(total.astype(BF))
    return out


def pool_step(t, turned_ref, y_ref, code_ref, pos_ref, scale_ref, xt_ref):
    for j in range(4):
        pool_table(t, j, turned_ref, y_ref, code_ref, scale_ref, xt_ref)
    return pool_pack(t, pos_ref, xt_ref)


def pool_body(tables_ref, ids_ref, out_ref, turned_ref, y_ref, code_ref, pos_ref, scale_ref, xt_ref):
    pool_turn(tables_ref, turned_ref)
    pool_setup(
        lambda q, j: ids_ref[pl.ds(q, 32, stride=4), j, :], y_ref, code_ref, pos_ref, scale_ref
    )

    def step(t, carry):
        blocks = pool_step(t, turned_ref, y_ref, code_ref, pos_ref, scale_ref, xt_ref)
        for half in range(2):
            out_ref[pl.ds(pl.multiple_of((2 * t + half) * 4 * ROOM, 4 * ROOM), 4 * ROOM), :] = blocks[half]
        return carry

    lax.fori_loop(0, 16, step, 0)


def pool_scratch():
    return [
        pltpu.VMEM((4, 16, 128, 128), BF),
        pltpu.VMEM((PLANE, 128), I32),
        pltpu.VMEM((4 * PLANE, 128), I32),
        pltpu.VMEM((128, 128), I32),
        pltpu.VMEM((128, 128), F32),
        pltpu.VMEM((2, 4, 128, 128), BF),
    ]


def order_columns(order_ref):
    slots = order_ref.shape[1]
    return onehot(iota((slots, slots), 0) == order_ref[...])


def weight_body(order_ref, top_ref, out_ref, raw_ref, plane_ref, perm_ref, sems):
    slots = out_ref.shape[2]
    copies = [
        pltpu.make_async_copy(top_ref.at[:, pl.ds(at * 128, 128)], raw_ref.at[at], sems.at[at]) for at in range(4)
    ]
    for copy in copies:
        copy.start()
    perm_ref[...] = order_columns(order_ref).astype(F32).T.astype(BF)
    for copy in copies:
        copy.wait()
    weight_cut(raw_ref, plane_ref)
    weight_turn(perm_ref, plane_ref, out_ref)


def weight_cut(raw_ref, plane_ref):
    row = iota((256, 256), 0)
    col = iota((256, 256), 1)
    spread = onehot((col % 16 == row // 16) & (col // 16 == row % 16))

    def cut(i, carry):
        for u in range(4):
            at = i * 4 + u
            rows = pl.ds(pl.multiple_of(at * 256, 256), 256)
            block = jnp.dot(
                spread, jnp.concatenate([raw_ref[c, rows, :] for c in range(4)], axis=1), preferred_element_type=F32
            ).astype(BF)
            for k in range(16):
                for c in range(4):
                    plane_ref[k, c, pl.ds(pl.multiple_of(at * 16, 16), 16), :] = block[
                        k * 16 : k * 16 + 16, c * 128 : c * 128 + 128
                    ]
        return carry

    lax.fori_loop(0, raw_ref.shape[1] // 1024, cut, 0)


def weight_turn(perm_ref, plane_ref, out_ref):
    perm = perm_ref[...]

    def turn(k, carry):
        plane = jnp.concatenate([plane_ref[k, c] for c in range(4)], axis=1)
        done = jnp.dot(perm, plane, preferred_element_type=F32).astype(BF)
        for c in range(4):
            out_ref[k, c] = done[:, c * 128 : c * 128 + 128]
        return carry

    lax.fori_loop(0, 16, turn, 0)


def weight_plane(k, perm_ref, plane_ref, raw_ref):
    plane = jnp.concatenate([plane_ref[k, c] for c in range(4)], axis=1)
    done = jnp.dot(perm_ref[...], plane, preferred_element_type=F32).astype(BF)
    for c in range(4):
        raw_ref[c, pl.ds(pl.multiple_of(k * 512, 512), 512), :] = done[:, c * 128 : c * 128 + 128]


def target_setup(inverse_ref, counts_ref, order_ref, compress_ref, turn_ref, mix_ref):
    samples, slots = inverse_ref.shape
    columns = order_columns(order_ref)
    mix_ref[...] = jnp.dot(compress_ref[...], columns, preferred_element_type=F32).astype(BF)
    chosen = jnp.dot(inverse_ref[...].astype(F32).astype(BF), columns, preferred_element_type=F32)
    counts = jnp.broadcast_to(counts_ref[...], (16, slots)).astype(F32)
    before = (iota((slots, slots), 0) // 4 == iota((slots, slots), 1) // 4) & (
        iota((slots, slots), 0) < iota((slots, slots), 1)
    )
    base = jnp.dot(counts.astype(BF), onehot(before), preferred_element_type=F32)[:1, :]
    offset = ((iota((1, slots), 1) // 4) % 2 * ROOM).astype(F32)
    place = jnp.where(chosen < counts[:1, :], chosen + (base + offset), 255.0)
    for at in range(slots // 128):
        turned = place[:, at * 128 : (at + 1) * 128].T.astype(I32).reshape(8, 16, 128)
        upper, lower = turned[:, :8].reshape(64, 128), turned[:, 8:].reshape(64, 128)
        two = upper | (lower << 8)
        turn_ref[pl.ds(at * 64, 64), :] = two | (pltpu.roll(two, 64, 1) << 16)


def pick_chunk(c, packed_ref, turn_ref, feat_ref):
    place = turn_ref[pl.ds(pl.multiple_of(c * 8, 8), 8), :]
    near = iota((16, 128), 1).astype(jnp.int16)
    far = near + jnp.int16(128)
    one, zero = jnp.ones((16, 128), BF), jnp.zeros((16, 128), BF)
    rows = jnp.concatenate(
        [packed_ref[pl.ds(pl.multiple_of(c * 320 + h * 160, 160), 160), :] for h in range(2)], axis=1
    )
    at = pl.ds(pl.multiple_of(c * 16, 16), 16)
    for part in range(4):
        left, right = [[], []], [[], []]
        for b in range(part * 16, part * 16 + 16):
            x = jnp.broadcast_to(place[:, b : b + 1], (8, 128))
            for v in range(2):
                cut = [(x >> (16 * v)) & 255, (x >> (16 * v + 8)) & 255]
                want = jnp.concatenate(cut, axis=0).astype(jnp.int16)
                left[v].append(jnp.where(want == near, one, zero))
                right[v].append(jnp.where(want == far, one, zero)[:, :32])
        got = jnp.dot(
            jnp.concatenate(
                [jnp.concatenate(left[0] + left[1], axis=0), jnp.concatenate(right[0] + right[1], axis=0)], axis=1
            ),
            rows,
            preferred_element_type=F32,
        ).reshape(2, 16, 16, 256)
        both = jnp.concatenate([got[:, :, :8, :128], got[:, :, 8:, 128:]], axis=2).astype(BF)
        for v in range(2):
            feat_ref[part * 16 : part * 16 + 16, v, at, :] = both[v]


def finish(feat_ref, mix_ref, weight_at, bias_ref, out_ref, left_ref, pair_ref, acc_ref):
    mix = mix_ref[...]
    zero = jnp.zeros((16, 128), BF)

    def mixing(i, carry):
        for u in range(8):
            feats = jnp.concatenate([feat_ref[i * 8 + u, v] for v in range(2)], axis=1)
            mixed = jnp.dot(mix, feats, preferred_element_type=F32).astype(BF)
            for v in range(2):
                left_ref[i * 8 + u, v, v * 16 : v * 16 + 16, :] = mixed[:, v * 128 : v * 128 + 128]
                left_ref[i * 8 + u, v, 16 - v * 16 : 32 - v * 16, :] = zero
        return carry

    lax.fori_loop(0, 8, mixing, 0)

    def pairing(i, carry):
        for u in range(8):
            sides = [
                jnp.concatenate([ref[i * 8 + u, v] for v in range(2)], axis=1) for ref in (left_ref, feat_ref)
            ]
            both = lax.dot_general(
                sides[0], sides[1], (((1,), (1,)), ((), ())), preferred_element_type=F32
            )
            for v in range(2):
                to = pl.ds(pl.multiple_of((v * 64 + i * 8 + u) * 24, 8), 16)
                for at in range(4):
                    pair_ref[at, to, :] = both[v * 16 : v * 16 + 16, at * 128 : at * 128 + 128]
        return carry

    lax.fori_loop(0, 8, pairing, 0)
    acc_ref[...] = jnp.broadcast_to(bias_ref[...], acc_ref.shape)

    def plane(i, carry):
        total = acc_ref[...]
        for u in range(4):
            k = i * 4 + u
            lhs = jnp.concatenate(
                [pair_ref[at, pl.ds(k, 128, stride=24), :].astype(BF) for at in range(4)], axis=1
            )
            total = total + jnp.dot(
                lhs, jnp.concatenate([weight_at(k, at) for at in range(4)], axis=1), preferred_element_type=F32)
        acc_ref[...] = total
        return carry

    lax.fori_loop(0, 4, plane, 0)
    out_ref[...] = jnp.maximum(acc_ref[...], 0.0).astype(BF)


def score_body(
    packed_ref, inverse_ref, counts_ref, order_ref, compress_ref, weight_ref, bias_ref,
    out_ref, turn_ref, mix_ref, feat_ref, left_ref, pair_ref, acc_ref,
):
    target_setup(inverse_ref, counts_ref, order_ref, compress_ref, turn_ref, mix_ref)

    def chunk(c, carry):
        pick_chunk(c, packed_ref, turn_ref, feat_ref)
        return carry

    lax.fori_loop(0, 32, chunk, 0)
    finish(feat_ref, mix_ref, lambda k, at: weight_ref[k, at], bias_ref, out_ref, left_ref, pair_ref, acc_ref)


def score_scratch():
    return [
        pltpu.VMEM((256, 128), I32),
        pltpu.VMEM((16, 512), BF),
        pltpu.VMEM((64, 2, 512, 128), BF),
        pltpu.VMEM((64, 2, 32, 128), BF),
        pltpu.VMEM((4, 3072, 128), F32),
        pltpu.VMEM((128, 512), F32),
    ]


VM = pl.BlockSpec(memory_space=pltpu.VMEM)
BIG = 60 * 1024 * 1024


def call(body, outs, scratch, count, flops, **kw):
    return pl.pallas_call(
        body,
        out_shape=outs,
        in_specs=[VM] * count,
        out_specs=VM,
        scratch_shapes=scratch,
        compiler_params=pltpu.CompilerParams(vmem_limit_bytes=BIG, **kw),
        cost_estimate=pl.CostEstimate(flops=flops, bytes_accessed=4 << 20, transcendentals=0),
    )


def weight_call(order, top):
    slots, units = order.shape[1], top.shape[1]
    shape = (16, units // 128, slots, 128)
    return pl.pallas_call(
        weight_body,
        out_shape=jax.ShapeDtypeStruct(shape, BF),
        in_specs=[VM, pl.BlockSpec(memory_space=pl.ANY)],
        out_specs=VM,
        scratch_shapes=[
            pltpu.VMEM((units // 128, top.shape[0], 128), BF),
            pltpu.VMEM(shape, BF),
            pltpu.VMEM((slots, slots), BF),
            pltpu.SemaphoreType.DMA((4,)),
        ],
        compiler_params=pltpu.CompilerParams(vmem_limit_bytes=BIG),
        cost_estimate=pl.CostEstimate(flops=6 * 10**9, bytes_accessed=16 << 20, transcendentals=0),
    )(order, top)


MESH = pl.DeviceIdType.MESH
GROUPS = 16


def lookup_body(
    rows_ref, lens_ref, counts_ref, inverse_ref, order_ref, compress_ref, bias_ref, tables_hbm, top_hbm,
    out_ref,
    tables_ref, turned_ref, y_ref, code_ref, pos_ref, scale_ref, xt_ref,
    raw_ref, plane_ref, perm_ref, ids_out, ids_in, ids_wide, send_ref, recv_ref,
    turn_ref, mix_ref, feat_ref, left_ref, pair_ref, acc_ref,
    local_sems, ids_sems, send_sem, recv_sems,
):
    n = 8 * GROUPS
    me = lax.axis_index("dev")
    my_group, my_place = me // 8, me % 8
    my_z, my_y = my_group // 2, my_group % 2

    barrier = pltpu.get_barrier_semaphore()

    def greet(i, carry):
        pl.semaphore_signal(barrier, 1, device_id={"dev": (me + i) % n}, device_id_type=MESH)
        return carry

    lax.fori_loop(1, n, greet, 0)
    copies = [pltpu.make_async_copy(tables_hbm, tables_ref, local_sems.at[4])] + [
        pltpu.make_async_copy(top_hbm.at[:, pl.ds(at * 128, 128)], raw_ref.at[at], local_sems.at[at])
        for at in range(4)
    ]
    for copy in copies:
        copy.start()

    prep_ids(rows_ref, lens_ref, counts_ref, ids_out)
    ids_in[me] = ids_out[me]
    pl.semaphore_wait(barrier, n - 1)

    def id_copy(src, dst, to):
        return pltpu.make_async_remote_copy(
            src_ref=src, dst_ref=dst, send_sem=ids_sems.at[0], recv_sem=ids_sems.at[1],
            device_id={"dev": to}, device_id_type=MESH,
        )

    def send_ids(i, carry):
        to = (me + i) % n
        id_copy(ids_out.at[to], ids_in.at[me], to).start()
        return carry

    lax.fori_loop(1, n, send_ids, 0)

    copies[0].wait()
    pool_turn(tables_ref, turned_ref)
    target_setup(inverse_ref, counts_ref, order_ref, compress_ref, turn_ref, mix_ref)
    perm_ref[...] = order_columns(order_ref).astype(F32).T.astype(BF)
    for copy in copies[1:]:
        copy.wait()
    weight_cut(raw_ref, plane_ref)

    everyone = id_copy(ids_out.at[pl.ds(0, n - 1)], ids_in.at[pl.ds(0, n - 1)], (me + 1) % n)
    everyone.wait_recv()
    ids_wide[...] = ids_in[...].astype(I32)
    pool_setup(
        lambda q, j: ids_wide[pl.ds(q, 32, stride=4), j, :], y_ref, code_ref, pos_ref, scale_ref
    )

    def shift(t):
        m = t // 2
        return 4 + ((m + 1) // 2) * (1 - 2 * (m % 2))

    def row_copy(src, dst, to, group):
        return pltpu.make_async_remote_copy(
            src_ref=src, dst_ref=dst, send_sem=send_sem.at[0], recv_sem=recv_sems.at[group],
            device_id={"dev": to}, device_id_type=MESH,
        )

    def block(ref, device):
        return ref.at[pl.ds(pl.multiple_of(device * ROOM, ROOM), ROOM), :]

    def target(t):
        return 2 * ((my_z + shift(t)) % 8) + (my_y + t) % 2

    def send_group(t):
        group = target(t)

        def one(i, carry):
            to = group * 8 + (my_place + i) % 8

            @pl.when(to != me)
            def _():
                row_copy(block(send_ref, to), block(recv_ref, me), to, my_group).start()

            return carry

        lax.fori_loop(0, 8, one, 0)

    def step(t, carry):
        group = target(t)
        pool_table(group, 0, turned_ref, y_ref, code_ref, scale_ref, xt_ref)

        @pl.when(t > 0)
        def _():
            send_group(t - 1)

        for j in range(1, 4):
            pool_table(group, j, turned_ref, y_ref, code_ref, scale_ref, xt_ref)
        blocks = pool_pack(group, pos_ref, xt_ref)
        for half in range(2):
            send_ref[pl.ds(pl.multiple_of((2 * group + half) * 4 * ROOM, 4 * ROOM), 4 * ROOM), :] = blocks[half]
        weight_plane(t, perm_ref, plane_ref, raw_ref)
        return carry

    lax.fori_loop(0, GROUPS, step, 0)
    send_group(GROUPS - 1)
    mine = pl.ds(pl.multiple_of(me * ROOM, ROOM), ROOM)
    recv_ref[mine, :] = send_ref[mine, :]

    def arrive(u, carry):
        group = 2 * ((my_z + 8 - shift(u)) % 8) + (my_y + u) % 2

        @pl.when(group == my_group)
        def _():
            rows = pl.ds(0, 7 * ROOM)
            row_copy(send_ref.at[rows, :], recv_ref.at[rows, :], (me + 1) % n, group).wait_recv()

        @pl.when(group != my_group)
        def _():
            rows = pl.ds(0, 8 * ROOM)
            row_copy(send_ref.at[rows, :], recv_ref.at[rows, :], (me + 1) % n, group).wait_recv()

        for v in range(2):
            pick_chunk(2 * group + v, recv_ref, turn_ref, feat_ref)
        return carry

    lax.fori_loop(0, GROUPS, arrive, 0)
    finish(
        feat_ref, mix_ref, lambda k, at: raw_ref[at, pl.ds(pl.multiple_of(k * 512, 512), 512), :],
        bias_ref, out_ref, left_ref, pair_ref, acc_ref,
    )
    everyone.wait_send()
    rows = pl.ds(0, (n - 1) * ROOM)
    row_copy(send_ref.at[rows, :], recv_ref.at[rows, :], (me + 1) % n, my_group).wait_send()


def shards(tables, bag_rows, bag_lengths, row_counts, inverse, table_order, compress, top_weight, top_bias):
    order = table_order.reshape(1, -1)
    bias = top_bias.reshape(1, -1)
    rows = bag_rows[0].transpose(1, 2, 0)
    lens = bag_lengths[0].transpose(1, 0)
    samples, units = inverse.shape[0], top_weight.shape[1]
    anywhere = pl.BlockSpec(memory_space=pl.ANY)
    scratch = (
        [pltpu.VMEM(tables.shape, BF)]
        + pool_scratch()
        + [
            pltpu.VMEM((units // 128, top_weight.shape[0], 128), BF),
            pltpu.VMEM((16, units // 128, 512, 128), BF),
            pltpu.VMEM((512, 512), BF),
            pltpu.VMEM((128, 4, 128), jnp.int16),
            pltpu.VMEM((128, 4, 128), jnp.int16),
            pltpu.VMEM((128, 4, 128), I32),
            pltpu.VMEM((128 * ROOM, 128), BF),
            pltpu.VMEM((128 * ROOM, 128), BF),
        ]
        + score_scratch()
        + [
            pltpu.SemaphoreType.DMA((5,)),
            pltpu.SemaphoreType.DMA((2,)),
            pltpu.SemaphoreType.DMA((1,)),
            pltpu.SemaphoreType.DMA((GROUPS,)),
        ]
    )
    return pl.pallas_call(
        lookup_body,
        out_shape=jax.ShapeDtypeStruct((samples, units), BF),
        in_specs=[VM] * 7 + [anywhere] * 2,
        out_specs=VM,
        scratch_shapes=scratch,
        compiler_params=pltpu.CompilerParams(vmem_limit_bytes=BIG, collective_id=0, has_side_effects=True),
        cost_estimate=pl.CostEstimate(flops=3 * 10**10, bytes_accessed=16 << 20, transcendentals=0),
    )(rows, lens, row_counts, inverse, order, compress, bias, tables, top_weight)


def solution(mesh):
    return jax.shard_map(
        shards,
        mesh=mesh,
        in_specs=(
            P("dev", None, None),
            P(("rep", "dev"), None, None, None),
            P(("rep", "dev"), None, None),
            P(("rep", "dev"), None),
            P(("rep", "dev"), None),
            P(),
            P(),
            P(),
            P(),
        ),
        out_specs=P(("rep", "dev"), None),
        check_vma=False,
    )
```

```python
import functools
import jax
import jax.numpy as jnp
from jax import lax
from jax.experimental import pallas as pl
from jax.experimental.pallas import tpu as pltpu
from jax.sharding import PartitionSpec as P

BF = jnp.bfloat16
F32 = jnp.float32
I32 = jnp.int32
ROOM = 80


def iota(shape, axis):
    return lax.broadcasted_iota(I32, shape, axis)


def onehot(mask):
    return jnp.where(mask, 1.0, 0.0).astype(BF)


def prep_ids(rows_ref, lens_ref, counts_ref, ids_out):
    most, pool, slots = rows_ref.shape
    used = iota((most, slots), 0) < counts_ref[...]
    lens = lens_ref[...]
    wide = jnp.concatenate(
        [jnp.where(used & (p < lens), rows_ref[:, p, :], -1) for p in range(pool)], axis=0
    )
    for at in range(slots // 128):
        turned = wide[:, at * 128 : (at + 1) * 128].T.reshape(32, 4, 128)
        ids_out[at * 32 : at * 32 + 32] = turned.astype(jnp.int16)


PLANE = 512


def pool_turn(tables_ref, turned_ref):
    tabs, vocab, width = tables_ref.shape
    for j in range(tabs):
        for at in range(vocab // 128):
            turned_ref[j, at] = (
                tables_ref[j, at * 128 : at * 128 + 128, :].astype(F32).T * (0.25 ** (at % 4))
            ).astype(BF)


def pool_setup(load_ids, y_ref, code_ref, pos_ref, scale_ref):
    lane = iota((32, 128), 1)
    chunk = lane // 32
    same = onehot(iota((128, 128), 0) // 32 == iota((128, 128), 1) // 32)
    base = jnp.zeros((32, 128), F32)
    for j in range(4):
        got = [load_ids(q, j) for q in range(4)]
        ys = []
        for p in range(4):
            y = got[0] if p == 0 else pltpu.roll(got[0], (-p * 32) % 128, 1)
            for q in range(1, 4):
                moved = got[q] if p == q else pltpu.roll(got[q], ((q - p) * 32) % 128, 1)
                y = jnp.where(chunk == q, moved, y)
            ys.append(y)
        valid = ys[0] >= 0
        total = jnp.dot(onehot(valid), same, preferred_element_type=F32)
        place = base.astype(I32) + (lane % 32) + chunk * ROOM
        pos_ref[pl.ds(j * 32, 32), :] = jnp.where(valid, place, -1)
        base = base + total
        alike = (ys[0] == ys[1]) & (ys[0] == ys[2]) & (ys[0] == ys[3])
        scale_ref[pl.ds(j * 32, 32), :] = jnp.where(alike, 2.0, 1.0)
        for p in range(4):
            y = ys[p]
            live = (y >= 0) if p < 2 else ((y >= 0) & ~alike)
            code = jnp.where(live, jnp.left_shift(jnp.ones_like(y), ((y >> 7) * 2) & 31), 0)
            y_ref[pl.ds((j * 4 + p) * 32, 32), :] = y & 127
            for k in range(4):
                code_ref[pl.ds(k * PLANE + (j * 4 + p) * 32, 32), :] = (
                    lax.shift_right_logical(code, jnp.full_like(code, 8 * k)) & 255
                )


def small(ref, at):
    return jnp.broadcast_to(ref[pl.ds(at, 1), :], (16, 128)).astype(jnp.int16)


def pool_table(t, j, turned_ref, y_ref, code_ref, scale_ref, xt_ref):
    low_iota = iota((16, 128), 0).astype(jnp.int16)
    zero = jnp.zeros((16, 128), jnp.int16)
    rows = [[(j * 4 + p) * 32 + 2 * t + half for p in range(4)] for half in range(2)]
    hits = []
    for half in range(2):
        lows = [small(y_ref, row) for row in rows[half]]
        hits.append([[low == low_iota + jnp.int16(16 * at) for low in lows] for at in range(8)])
    total = None
    for k in range(4):
        planes = []
        for half in range(2):
            codes = [small(code_ref, k * PLANE + row) for row in rows[half]]
            plane = []
            for hit in hits[half]:
                cut = [jnp.where(hit[p], codes[p], zero) for p in range(4)]
                plane.append((cut[0] + cut[1]) + (cut[2] + cut[3]))
            planes.append(jnp.concatenate(plane, axis=0).astype(jnp.uint8))
        for i in (0, 2):
            hot = jnp.concatenate(
                [
                    jnp.concatenate([(plane & jnp.uint8(3 << (2 * u))).astype(BF) for u in (i, i + 1)], axis=0)
                    for plane in planes
                ],
                axis=1,
            )
            left = jnp.concatenate([turned_ref[j, 4 * k + i], turned_ref[j, 4 * k + i + 1]], axis=1)
            part = jnp.dot(left, hot, preferred_element_type=F32)
            total = part if total is None else total + part
    for half in range(2):
        scale = scale_ref[pl.ds(j * 32 + 2 * t + half, 1), :]
        xt_ref[half, j] = (total[:, half * 128 : half * 128 + 128] * scale).astype(BF)


def pool_pack(t, pos_ref, xt_ref):
    out = []
    for half in range(2):
        total = None
        for jj in range(2):
            packs, cols = [], []
            for j in (2 * jj, 2 * jj + 1):
                pos = small(pos_ref, j * 32 + 2 * t + half)
                hits = [
                    jnp.where(
                        pos == iota((16, 128), 0).astype(jnp.int16) + jnp.int16(16 * at),
                        jnp.ones((16, 128), BF),
                        jnp.zeros((16, 128), BF),
                    )
                    for at in range(4 * ROOM // 16)
                ]
                packs.append(jnp.concatenate(hits, axis=0))
                cols.append(xt_ref[half, j])
            part = lax.dot_general(
                jnp.concatenate(packs, axis=1),
                jnp.concatenate(cols, axis=1),
                (((1,), (1,)), ((), ())),
                preferred_element_type=F32,
            )
            total = part if total is None else total + part
        out.append(total.astype(BF))
    return out


def pool_step(t, turned_ref, y_ref, code_ref, pos_ref, scale_ref, xt_ref):
    for j in range(4):
        pool_table(t, j, turned_ref, y_ref, code_ref, scale_ref, xt_ref)
    return pool_pack(t, pos_ref, xt_ref)


def pool_scratch():
    return [
        pltpu.VMEM((4, 16, 128, 128), BF),
        pltpu.VMEM((PLANE, 128), I32),
        pltpu.VMEM((4 * PLANE, 128), I32),
        pltpu.VMEM((128, 128), I32),
        pltpu.VMEM((128, 128), F32),
        pltpu.VMEM((2, 4, 128, 128), BF),
    ]


def order_columns(order_ref):
    slots = order_ref.shape[1]
    return onehot(iota((slots, slots), 0) == order_ref[...])


def weight_cut(at, raw_ref, plane_ref):
    row = iota((256, 256), 0)
    col = iota((256, 256), 1)
    spread = onehot((col % 16 == row // 16) & (col // 16 == row % 16))
    rows = pl.ds(pl.multiple_of(at * 256, 256), 256)
    block = jnp.dot(
        spread, jnp.concatenate([raw_ref[c, rows, :] for c in range(4)], axis=1), preferred_element_type=F32
    ).astype(BF)
    for k in range(16):
        for c in range(4):
            plane_ref[k, c, pl.ds(pl.multiple_of(at * 16, 16), 16), :] = block[
                k * 16 : k * 16 + 16, c * 128 : c * 128 + 128
            ]


def weight_plane(k, perm_ref, plane_ref, raw_ref):
    plane = jnp.concatenate([plane_ref[k, c] for c in range(4)], axis=1)
    done = jnp.dot(perm_ref[...], plane, preferred_element_type=F32).astype(BF)
    for c in range(4):
        raw_ref[c, pl.ds(pl.multiple_of(k * 512, 512), 512), :] = done[:, c * 128 : c * 128 + 128]


def target_setup(inverse_ref, counts_ref, order_ref, compress_ref, turn_ref, mix_ref):
    samples, slots = inverse_ref.shape
    columns = order_columns(order_ref)
    mix_ref[...] = jnp.dot(compress_ref[...], columns, preferred_element_type=F32).astype(BF)
    chosen = jnp.dot(inverse_ref[...].astype(F32).astype(BF), columns, preferred_element_type=F32)
    counts = jnp.broadcast_to(counts_ref[...], (16, slots)).astype(F32)
    before = (iota((slots, slots), 0) // 4 == iota((slots, slots), 1) // 4) & (
        iota((slots, slots), 0) < iota((slots, slots), 1)
    )
    base = jnp.dot(counts.astype(BF), onehot(before), preferred_element_type=F32)[:1, :]
    offset = ((iota((1, slots), 1) // 4) % 2 * ROOM).astype(F32)
    place = jnp.where(chosen < counts[:1, :], chosen + (base + offset), 255.0)
    for at in range(slots // 128):
        turned = place[:, at * 128 : (at + 1) * 128].T.astype(I32).reshape(8, 16, 128)
        upper, lower = turned[:, :8].reshape(64, 128), turned[:, 8:].reshape(64, 128)
        two = upper | (lower << 8)
        turn_ref[pl.ds(at * 64, 64), :] = two | (pltpu.roll(two, 64, 1) << 16)


def pick_chunk(c, packed_ref, turn_ref, feat_ref):
    place = turn_ref[pl.ds(pl.multiple_of(c * 8, 8), 8), :]
    near = iota((16, 128), 1).astype(jnp.int16)
    far = near + jnp.int16(128)
    one, zero = jnp.ones((16, 128), BF), jnp.zeros((16, 128), BF)
    rows = jnp.concatenate(
        [packed_ref[pl.ds(pl.multiple_of(c * 320 + h * 160, 160), 160), :] for h in range(2)], axis=1
    )
    at = pl.ds(pl.multiple_of(c * 16, 16), 16)
    for part in range(4):
        left, right = [[], []], [[], []]
        for b in range(part * 16, part * 16 + 16):
            x = jnp.broadcast_to(place[:, b : b + 1], (8, 128))
            for v in range(2):
                cut = [(x >> (16 * v)) & 255, (x >> (16 * v + 8)) & 255]
                want = jnp.concatenate(cut, axis=0).astype(jnp.int16)
                left[v].append(jnp.where(want == near, one, zero))
                right[v].append(jnp.where(want == far, one, zero)[:, :32])
        got = jnp.dot(
            jnp.concatenate(
                [jnp.concatenate(left[0] + left[1], axis=0), jnp.concatenate(right[0] + right[1], axis=0)], axis=1
            ),
            rows,
            preferred_element_type=F32,
        ).reshape(2, 16, 16, 256)
        both = jnp.concatenate([got[:, :, :8, :128], got[:, :, 8:, 128:]], axis=2).astype(BF)
        for v in range(2):
            feat_ref[part * 16 : part * 16 + 16, v, at, :] = both[v]


def mixing(columns, feats_of, store):
    def some(i, carry):
        for u in range(8):
            feats = jnp.concatenate([feats_of(i * 8 + u, v) for v in range(2)], axis=1)
            store(i * 8 + u, jnp.dot(columns, feats, preferred_element_type=F32))
        return carry

    lax.fori_loop(0, 8, some, 0)


def finish(feat_ref, weight_at, bias_ref, out_ref, left_ref, pair_ref, acc_ref):
    def pairing(i, carry):
        for u in range(8):
            sides = [
                jnp.concatenate([ref[i * 8 + u, v] for v in range(2)], axis=1) for ref in (left_ref, feat_ref)
            ]
            both = lax.dot_general(
                sides[0], sides[1], (((1,), (1,)), ((), ())), preferred_element_type=F32
            )
            for v in range(2):
                to = pl.ds(pl.multiple_of((v * 64 + i * 8 + u) * 24, 8), 16)
                for at in range(4):
                    pair_ref[at, to, :] = both[v * 16 : v * 16 + 16, at * 128 : at * 128 + 128]
        return carry

    lax.fori_loop(0, 8, pairing, 0)
    acc_ref[...] = jnp.broadcast_to(bias_ref[...], acc_ref.shape)

    def plane(i, carry):
        total = acc_ref[...]
        for u in range(4):
            k = i * 4 + u
            lhs = jnp.concatenate(
                [pair_ref[at, pl.ds(k, 128, stride=24), :].astype(BF) for at in range(4)], axis=1
            )
            total = total + jnp.dot(
                lhs, jnp.concatenate([weight_at(k, at) for at in range(4)], axis=1), preferred_element_type=F32)
        acc_ref[...] = total
        return carry

    lax.fori_loop(0, 4, plane, 0)
    out_ref[...] = jnp.maximum(acc_ref[...], 0.0).astype(BF)


def score_scratch():
    return [
        pltpu.VMEM((256, 128), I32),
        pltpu.VMEM((16, 512), BF),
        pltpu.VMEM((64, 2, 512, 128), BF),
        pltpu.VMEM((64, 2, 32, 128), BF),
        pltpu.VMEM((64, 16, 256), F32),
        pltpu.VMEM((4, 3072, 128), F32),
        pltpu.VMEM((128, 512), F32),
    ]


VM = pl.BlockSpec(memory_space=pltpu.VMEM)
BIG = 60 * 1024 * 1024


MESH = pl.DeviceIdType.MESH
GROUPS = 16


def lookup_body(
    rows_ref, lens_ref, counts_ref, inverse_ref, order_ref, compress_ref, bias_ref, tables_hbm, top_hbm,
    out_ref,
    tables_ref, turned_ref, y_ref, code_ref, pos_ref, scale_ref, xt_ref,
    raw_ref, plane_ref, perm_ref, ids_out, ids_in, ids_wide, send_ref, recv_ref,
    turn_ref, mix_ref, feat_ref, left_ref, sum_ref, pair_ref, acc_ref, cols_ref,
    local_sems, ids_sems, send_sem, recv_sems,
):
    n = 8 * GROUPS
    me = lax.axis_index("dev")
    my_group, my_place, my_chunk = me // 8, me % 8, me // 4
    my_z, my_y = my_group // 2, my_group % 2

    def shift(t):
        m = t // 2
        m = m - jnp.where(m > 3, 1, 0)
        far = 4 + ((m + 1) // 2) * (1 - 2 * (m % 2))
        return jnp.where(t // 2 == 3, 0, far)

    def target(t):
        return 2 * ((my_z + shift(t)) % 8) + (my_y + t) % 2

    def each_other(act):
        def some(t, carry):
            def one(i, inner):
                to = target(t) * 8 + (my_place + i) % 8

                @pl.when(to != me)
                def _():
                    act(to)

                return inner

            return lax.fori_loop(0, 8, one, carry)

        lax.fori_loop(0, GROUPS, some, 0)

    barrier = pltpu.get_barrier_semaphore()
    each_other(lambda to: pl.semaphore_signal(barrier, 1, device_id={"dev": to}, device_id_type=MESH))
    copies = [pltpu.make_async_copy(tables_hbm, tables_ref, local_sems.at[4])] + [
        pltpu.make_async_copy(top_hbm.at[:, pl.ds(at * 128, 128)], raw_ref.at[at], local_sems.at[at])
        for at in range(4)
    ]
    for copy in copies:
        copy.start()

    prep_ids(rows_ref, lens_ref, counts_ref, ids_out)
    ids_in[me] = ids_out[me]
    target_setup(inverse_ref, counts_ref, order_ref, compress_ref, turn_ref, mix_ref)
    copies[0].wait()
    pool_turn(tables_ref, turned_ref)
    pl.semaphore_wait(barrier, n - 1)

    def id_copy(src, dst, to):
        return pltpu.make_async_remote_copy(
            src_ref=src, dst_ref=dst, send_sem=ids_sems.at[0], recv_sem=ids_sems.at[1],
            device_id={"dev": to}, device_id_type=MESH,
        )

    each_other(lambda to: id_copy(ids_out.at[to], ids_in.at[me], to).start())
    perm_ref[...] = order_columns(order_ref).astype(F32).T.astype(BF)
    for g in range(GROUPS):
        cols_ref[g] = mix_ref[:, g * 32 : g * 32 + 32]

    def clear(g, carry):
        rows = pl.ds(pl.multiple_of(arrived(GROUPS - 4 + g) * 32, 32), 32)
        feat_ref[:, :, rows, :] = jnp.zeros((64, 2, 32, 128), BF)
        return carry

    def arrived(u):
        return 2 * ((my_z + 8 - shift(u)) % 8) + (my_y + u) % 2

    lax.fori_loop(0, 4, clear, 0)
    for copy in copies[1:]:
        copy.wait()

    everyone = id_copy(ids_out.at[pl.ds(0, n - 1)], ids_in.at[pl.ds(0, n - 1)], (me + 1) % n)
    everyone.wait_recv()
    ids_wide[...] = ids_in[...].astype(I32)
    pool_setup(
        lambda q, j: ids_wide[pl.ds(q, 32, stride=4), j, :], y_ref, code_ref, pos_ref, scale_ref
    )

    def row_copy(src, dst, to, chunk):
        return pltpu.make_async_remote_copy(
            src_ref=src, dst_ref=dst, send_sem=send_sem.at[0], recv_sem=recv_sems.at[chunk],
            device_id={"dev": to}, device_id_type=MESH,
        )

    def block(ref, device):
        return ref.at[pl.ds(pl.multiple_of(device * ROOM, ROOM), ROOM), :]

    def step(t, carry):
        group = target(t)
        for j in range(4):
            pool_table(group, j, turned_ref, y_ref, code_ref, scale_ref, xt_ref)
        blocks = pool_pack(group, pos_ref, xt_ref)
        for half in range(2):
            send_ref[pl.ds(pl.multiple_of((2 * group + half) * 4 * ROOM, 4 * ROOM), 4 * ROOM), :] = blocks[half]
        for u in range(2):
            weight_cut(2 * t + u, raw_ref, plane_ref)

        def one(i, inner):
            to = group * 8 + (my_place + i) % 8

            @pl.when(to != me)
            def _():
                row_copy(block(send_ref, to), block(recv_ref, me), to, my_chunk).start()

            return inner

        lax.fori_loop(0, 8, one, 0)
        return carry

    lax.fori_loop(0, GROUPS, step, 0)
    mine = pl.ds(pl.multiple_of(me * ROOM, ROOM), ROOM)
    recv_ref[mine, :] = send_ref[mine, :]

    def take(u, carry):
        group = arrived(u)

        def half(v, inner):
            chunk = 2 * group + (my_chunk + v) % 2

            @pl.when(chunk == my_chunk)
            def _():
                rows = pl.ds(0, 3 * ROOM)
                row_copy(send_ref.at[rows, :], recv_ref.at[rows, :], (me + 1) % n, chunk).wait_recv()

            @pl.when(chunk != my_chunk)
            def _():
                rows = pl.ds(0, 4 * ROOM)
                row_copy(send_ref.at[rows, :], recv_ref.at[rows, :], (me + 1) % n, chunk).wait_recv()

            pick_chunk(chunk, recv_ref, turn_ref, feat_ref)
            return inner

        return lax.fori_loop(0, 2, half, carry)

    def turn_and_take(u, carry):
        for k in range(2):
            weight_plane(2 * u + k, perm_ref, plane_ref, raw_ref)
        return take(u, carry)

    lax.fori_loop(0, 8, turn_and_take, 0)
    lax.fori_loop(8, GROUPS - 4, take, 0)

    def keep(i, value):
        sum_ref[i] = value

    mixing(mix_ref[...], lambda i, v: feat_ref[i, v], keep)
    lax.fori_loop(GROUPS - 4, GROUPS, take, 0)
    last = [arrived(GROUPS - 4 + g) for g in range(4)]
    zero = jnp.zeros((16, 128), BF)

    def settle(i, value):
        mixed = (sum_ref[i] + value).astype(BF)
        for v in range(2):
            left_ref[i, v, v * 16 : v * 16 + 16, :] = mixed[:, v * 128 : v * 128 + 128]
            left_ref[i, v, 16 - v * 16 : 32 - v * 16, :] = zero

    mixing(
        jnp.concatenate([cols_ref[g] for g in last], axis=1),
        lambda i, v: jnp.concatenate(
            [feat_ref[i, v, pl.ds(pl.multiple_of(g * 32, 32), 32), :] for g in last], axis=0
        ),
        settle,
    )
    finish(
        feat_ref, lambda k, at: raw_ref[at, pl.ds(pl.multiple_of(k * 512, 512), 512), :],
        bias_ref, out_ref, left_ref, pair_ref, acc_ref,
    )
    everyone.wait_send()
    rows = pl.ds(0, (n - 1) * ROOM)
    row_copy(send_ref.at[rows, :], recv_ref.at[rows, :], (me + 1) % n, my_chunk).wait_send()


def shards(tables, bag_rows, bag_lengths, row_counts, inverse, table_order, compress, top_weight, top_bias):
    order = table_order.reshape(1, -1)
    bias = top_bias.reshape(1, -1)
    rows = bag_rows[0].transpose(1, 2, 0)
    lens = bag_lengths[0].transpose(1, 0)
    samples, units = inverse.shape[0], top_weight.shape[1]
    anywhere = pl.BlockSpec(memory_space=pl.ANY)
    scratch = (
        [pltpu.VMEM(tables.shape, BF)]
        + pool_scratch()
        + [
            pltpu.VMEM((units // 128, top_weight.shape[0], 128), BF),
            pltpu.VMEM((16, units // 128, 512, 128), BF),
            pltpu.VMEM((512, 512), BF),
            pltpu.VMEM((128, 4, 128), jnp.int16),
            pltpu.VMEM((128, 4, 128), jnp.int16),
            pltpu.VMEM((128, 4, 128), I32),
            pltpu.VMEM((128 * ROOM, 128), BF),
            pltpu.VMEM((128 * ROOM, 128), BF),
        ]
        + score_scratch()
        + [pltpu.VMEM((GROUPS, 16, 32), BF)]
        + [
            pltpu.SemaphoreType.DMA((5,)),
            pltpu.SemaphoreType.DMA((2,)),
            pltpu.SemaphoreType.DMA((1,)),
            pltpu.SemaphoreType.DMA((2 * GROUPS,)),
        ]
    )
    return pl.pallas_call(
        lookup_body,
        out_shape=jax.ShapeDtypeStruct((samples, units), BF),
        in_specs=[VM] * 7 + [anywhere] * 2,
        out_specs=VM,
        scratch_shapes=scratch,
        compiler_params=pltpu.CompilerParams(vmem_limit_bytes=BIG, collective_id=0, has_side_effects=True),
        cost_estimate=pl.CostEstimate(flops=3 * 10**10, bytes_accessed=16 << 20, transcendentals=0),
    )(rows, lens, row_counts, inverse, order, compress, bias, tables, top_weight)


def solution(mesh):
    return jax.shard_map(
        shards,
        mesh=mesh,
        in_specs=(
            P("dev", None, None),
            P(("rep", "dev"), None, None, None),
            P(("rep", "dev"), None, None),
            P(("rep", "dev"), None),
            P(("rep", "dev"), None),
            P(),
            P(),
            P(),
            P(),
        ),
        out_specs=P(("rep", "dev"), None),
        check_vma=False,
    )
```

```python
import functools
import jax
import jax.numpy as jnp
from jax import lax
from jax.experimental import pallas as pl
from jax.experimental.pallas import tpu as pltpu
from jax.sharding import PartitionSpec as P

BF = jnp.bfloat16
F32 = jnp.float32
I32 = jnp.int32
ROOM = 80


def iota(shape, axis):
    return lax.broadcasted_iota(I32, shape, axis)


def onehot(mask):
    return jnp.where(mask, 1.0, 0.0).astype(BF)


def prep_ids(rows_ref, lens_ref, counts_ref, ids_out):
    most, pool, slots = rows_ref.shape
    used = iota((most, slots), 0) < counts_ref[...]
    lens = lens_ref[...]
    wide = jnp.concatenate(
        [jnp.where(used & (p < lens), rows_ref[:, p, :], -1) for p in range(pool)], axis=0
    )
    for at in range(slots // 128):
        turned = wide[:, at * 128 : (at + 1) * 128].T.reshape(32, 4, 128)
        ids_out[at * 32 : at * 32 + 32] = turned.astype(jnp.int16)


PLANE = 512


def pool_turn(tables_ref, turned_ref):
    tabs, vocab, width = tables_ref.shape
    for j in range(tabs):
        for at in range(vocab // 128):
            turned_ref[j, at] = (
                tables_ref[j, at * 128 : at * 128 + 128, :].astype(F32).T * (0.25 ** (at % 4))
            ).astype(BF)


def pool_setup(load_ids, y_ref, code_ref, pos_ref, scale_ref):
    lane = iota((32, 128), 1)
    chunk = lane // 32
    same = onehot(iota((128, 128), 0) // 32 == iota((128, 128), 1) // 32)
    base = jnp.zeros((32, 128), F32)
    for j in range(4):
        got = [load_ids(q, j) for q in range(4)]
        ys = []
        for p in range(4):
            y = got[0] if p == 0 else pltpu.roll(got[0], (-p * 32) % 128, 1)
            for q in range(1, 4):
                moved = got[q] if p == q else pltpu.roll(got[q], ((q - p) * 32) % 128, 1)
                y = jnp.where(chunk == q, moved, y)
            ys.append(y)
        valid = ys[0] >= 0
        total = jnp.dot(onehot(valid), same, preferred_element_type=F32)
        place = base.astype(I32) + (lane % 32) + chunk * ROOM
        pos_ref[pl.ds(j * 32, 32), :] = jnp.where(valid, place, -1)
        base = base + total
        alike = (ys[0] == ys[1]) & (ys[0] == ys[2]) & (ys[0] == ys[3])
        scale_ref[pl.ds(j * 32, 32), :] = jnp.where(alike, 2.0, 1.0)
        for p in range(4):
            y = ys[p]
            live = (y >= 0) if p < 2 else ((y >= 0) & ~alike)
            code = jnp.where(live, jnp.left_shift(jnp.ones_like(y), ((y >> 7) * 2) & 31), 0)
            y_ref[pl.ds((j * 4 + p) * 32, 32), :] = y & 127
            for k in range(4):
                code_ref[pl.ds(k * PLANE + (j * 4 + p) * 32, 32), :] = (
                    lax.shift_right_logical(code, jnp.full_like(code, 8 * k)) & 255
                )


def small(ref, at):
    return jnp.broadcast_to(ref[pl.ds(at, 1), :], (16, 128)).astype(jnp.int16)


def pool_table(t, j, turned_ref, y_ref, code_ref, scale_ref, xt_ref):
    low_iota = iota((16, 128), 0).astype(jnp.int16)
    zero = jnp.zeros((16, 128), jnp.int16)
    rows = [[(j * 4 + p) * 32 + 2 * t + half for p in range(4)] for half in range(2)]
    hits = []
    for half in range(2):
        lows = [small(y_ref, row) for row in rows[half]]
        hits.append([[low == low_iota + jnp.int16(16 * at) for low in lows] for at in range(8)])
    total = None
    for k in range(4):
        planes = []
        for half in range(2):
            codes = [small(code_ref, k * PLANE + row) for row in rows[half]]
            plane = []
            for hit in hits[half]:
                cut = [jnp.where(hit[p], codes[p], zero) for p in range(4)]
                plane.append((cut[0] + cut[1]) + (cut[2] + cut[3]))
            planes.append(jnp.concatenate(plane, axis=0).astype(jnp.uint8))
        for i in (0, 2):
            hot = jnp.concatenate(
                [
                    jnp.concatenate([(plane & jnp.uint8(3 << (2 * u))).astype(BF) for u in (i, i + 1)], axis=0)
                    for plane in planes
                ],
                axis=1,
            )
            left = jnp.concatenate([turned_ref[j, 4 * k + i], turned_ref[j, 4 * k + i + 1]], axis=1)
            part = jnp.dot(left, hot, preferred_element_type=F32)
            total = part if total is None else total + part
    for half in range(2):
        scale = scale_ref[pl.ds(j * 32 + 2 * t + half, 1), :]
        xt_ref[half, j] = (total[:, half * 128 : half * 128 + 128] * scale).astype(BF)


def pool_pack(t, pos_ref, xt_ref):
    out = []
    for half in range(2):
        total = None
        for jj in range(2):
            packs, cols = [], []
            for j in (2 * jj, 2 * jj + 1):
                pos = small(pos_ref, j * 32 + 2 * t + half)
                hits = [
                    jnp.where(
                        pos == iota((16, 128), 0).astype(jnp.int16) + jnp.int16(16 * at),
                        jnp.ones((16, 128), BF),
                        jnp.zeros((16, 128), BF),
                    )
                    for at in range(4 * ROOM // 16)
                ]
                packs.append(jnp.concatenate(hits, axis=0))
                cols.append(xt_ref[half, j])
            part = lax.dot_general(
                jnp.concatenate(packs, axis=1),
                jnp.concatenate(cols, axis=1),
                (((1,), (1,)), ((), ())),
                preferred_element_type=F32,
            )
            total = part if total is None else total + part
        out.append(total.astype(BF))
    return out


def pool_step(t, turned_ref, y_ref, code_ref, pos_ref, scale_ref, xt_ref):
    for j in range(4):
        pool_table(t, j, turned_ref, y_ref, code_ref, scale_ref, xt_ref)
    return pool_pack(t, pos_ref, xt_ref)


def pool_scratch():
    return [
        pltpu.VMEM((4, 16, 128, 128), BF),
        pltpu.VMEM((PLANE, 128), I32),
        pltpu.VMEM((4 * PLANE, 128), I32),
        pltpu.VMEM((128, 128), I32),
        pltpu.VMEM((128, 128), F32),
        pltpu.VMEM((2, 4, 128, 128), BF),
    ]


def order_columns(order_ref):
    slots = order_ref.shape[1]
    return onehot(iota((slots, slots), 0) == order_ref[...])


def weight_cut(at, raw_ref, plane_ref):
    row = iota((256, 256), 0)
    col = iota((256, 256), 1)
    spread = onehot((col % 16 == row // 16) & (col // 16 == row % 16))
    rows = pl.ds(pl.multiple_of(at * 256, 256), 256)
    block = jnp.dot(
        spread, jnp.concatenate([raw_ref[c, rows, :] for c in range(4)], axis=1), preferred_element_type=F32
    ).astype(BF)
    for k in range(16):
        for c in range(4):
            plane_ref[k, c, pl.ds(pl.multiple_of(at * 16, 16), 16), :] = block[
                k * 16 : k * 16 + 16, c * 128 : c * 128 + 128
            ]


def weight_plane(k, perm_ref, plane_ref, raw_ref):
    plane = jnp.concatenate([plane_ref[k, c] for c in range(4)], axis=1)
    done = jnp.dot(perm_ref[...], plane, preferred_element_type=F32).astype(BF)
    for c in range(4):
        raw_ref[c, pl.ds(pl.multiple_of(k * 512, 512), 512), :] = done[:, c * 128 : c * 128 + 128]


def target_setup(inverse_ref, counts_ref, order_ref, compress_ref, turn_ref, mix_ref):
    samples, slots = inverse_ref.shape
    columns = order_columns(order_ref)
    mix_ref[...] = jnp.dot(compress_ref[...], columns, preferred_element_type=F32).astype(BF)
    chosen = jnp.dot(inverse_ref[...].astype(F32).astype(BF), columns, preferred_element_type=F32)
    counts = jnp.broadcast_to(counts_ref[...], (16, slots)).astype(F32)
    before = (iota((slots, slots), 0) // 4 == iota((slots, slots), 1) // 4) & (
        iota((slots, slots), 0) < iota((slots, slots), 1)
    )
    base = jnp.dot(counts.astype(BF), onehot(before), preferred_element_type=F32)[:1, :]
    offset = ((iota((1, slots), 1) // 4) % 2 * ROOM).astype(F32)
    place = jnp.where(chosen < counts[:1, :], chosen + (base + offset), 255.0)
    for at in range(slots // 128):
        turned = place[:, at * 128 : (at + 1) * 128].T.astype(I32).reshape(8, 16, 128)
        upper, lower = turned[:, :8].reshape(64, 128), turned[:, 8:].reshape(64, 128)
        two = upper | (lower << 8)
        turn_ref[pl.ds(at * 64, 64), :] = two | (pltpu.roll(two, 64, 1) << 16)


def pick_chunk(c, packed_ref, turn_ref, feat_ref):
    place = turn_ref[pl.ds(pl.multiple_of(c * 8, 8), 8), :]
    near = iota((16, 128), 1).astype(jnp.int16)
    far = near + jnp.int16(128)
    one, zero = jnp.ones((16, 128), BF), jnp.zeros((16, 128), BF)
    rows = jnp.concatenate(
        [packed_ref[pl.ds(pl.multiple_of(c * 320 + h * 160, 160), 160), :] for h in range(2)], axis=1
    )
    at = pl.ds(pl.multiple_of(c * 16, 16), 16)
    for part in range(4):
        left, right = [[], []], [[], []]
        for b in range(part * 16, part * 16 + 16):
            x = jnp.broadcast_to(place[:, b : b + 1], (8, 128))
            for v in range(2):
                cut = [(x >> (16 * v)) & 255, (x >> (16 * v + 8)) & 255]
                want = jnp.concatenate(cut, axis=0).astype(jnp.int16)
                left[v].append(jnp.where(want == near, one, zero))
                right[v].append(jnp.where(want == far, one, zero)[:, :32])
        got = jnp.dot(
            jnp.concatenate(
                [jnp.concatenate(left[0] + left[1], axis=0), jnp.concatenate(right[0] + right[1], axis=0)], axis=1
            ),
            rows,
            preferred_element_type=F32,
        ).reshape(2, 16, 16, 256)
        both = jnp.concatenate([got[:, :, :8, :128], got[:, :, 8:, 128:]], axis=2).astype(BF)
        for v in range(2):
            feat_ref[part * 16 : part * 16 + 16, v, at, :] = both[v]


def mixing(columns, feats_of, store):
    def some(i, carry):
        for u in range(8):
            feats = jnp.concatenate([feats_of(i * 8 + u, v) for v in range(2)], axis=1)
            store(i * 8 + u, jnp.dot(columns, feats, preferred_element_type=F32))
        return carry

    lax.fori_loop(0, 8, some, 0)


def finish(feat_ref, weight_at, bias_ref, out_ref, left_ref, pair_ref, acc_ref):
    def pairing(i, carry):
        for u in range(8):
            sides = [
                jnp.concatenate([ref[i * 8 + u, v] for v in range(2)], axis=1) for ref in (left_ref, feat_ref)
            ]
            both = lax.dot_general(
                sides[0], sides[1], (((1,), (1,)), ((), ())), preferred_element_type=F32
            )
            for v in range(2):
                to = pl.ds(pl.multiple_of((v * 64 + i * 8 + u) * 24, 8), 16)
                for at in range(4):
                    pair_ref[at, to, :] = both[v * 16 : v * 16 + 16, at * 128 : at * 128 + 128]
        return carry

    lax.fori_loop(0, 8, pairing, 0)
    acc_ref[...] = jnp.broadcast_to(bias_ref[...], acc_ref.shape)

    def plane(i, carry):
        total = acc_ref[...]
        for u in range(4):
            k = i * 4 + u
            lhs = jnp.concatenate(
                [pair_ref[at, pl.ds(k, 128, stride=24), :].astype(BF) for at in range(4)], axis=1
            )
            total = total + jnp.dot(
                lhs, jnp.concatenate([weight_at(k, at) for at in range(4)], axis=1), preferred_element_type=F32)
        acc_ref[...] = total
        return carry

    lax.fori_loop(0, 4, plane, 0)
    out_ref[...] = acc_ref[...]


def score_scratch():
    return [
        pltpu.VMEM((256, 128), I32),
        pltpu.VMEM((16, 512), BF),
        pltpu.VMEM((64, 2, 512, 128), BF),
        pltpu.VMEM((64, 2, 32, 128), BF),
        pltpu.VMEM((64, 16, 256), F32),
        pltpu.VMEM((4, 3072, 128), F32),
        pltpu.VMEM((128, 512), F32),
    ]


VM = pl.BlockSpec(memory_space=pltpu.VMEM)
BIG = 56 * 1024 * 1024


MESH = pl.DeviceIdType.MESH
GROUPS = 16


def lookup_body(
    rows_ref, lens_ref, counts_ref, inverse_ref, order_ref, compress_ref, bias_ref, tables_hbm, top_hbm,
    out_ref,
    tables_ref, turned_ref, y_ref, code_ref, pos_ref, scale_ref, xt_ref,
    raw_ref, plane_ref, perm_ref, ids_out, ids_in, ids_wide, send_ref, recv_ref,
    turn_ref, mix_ref, feat_ref, left_ref, sum_ref, pair_ref, acc_ref, cols_ref,
    local_sems, ids_sems, send_sem, recv_sems,
):
    n = 8 * GROUPS
    me = lax.axis_index("dev")
    my_group, my_place, my_chunk = me // 8, me % 8, me // 4
    my_z, my_y = my_group // 2, my_group % 2

    def shift(t):
        m = t // 2
        m = m - jnp.where(m > 3, 1, 0)
        far = 4 + ((m + 1) // 2) * (1 - 2 * (m % 2))
        return jnp.where(t // 2 == 3, 0, far)

    def target(t):
        return 2 * ((my_z + shift(t)) % 8) + (my_y + t) % 2

    def each_other(act):
        def some(t, carry):
            for i in range(8):
                act((me + n // 2 + t * 8 + i) & (n - 1))
            return carry

        lax.fori_loop(0, n // 16, some, 0)
        for i in range(1, 8):
            act((me + i) & (n - 1))
        lax.fori_loop(n // 16 + 1, n // 8, some, 0)

    barrier = pltpu.get_barrier_semaphore()
    each_other(lambda to: pl.semaphore_signal(barrier, 1, device_id={"dev": to}, device_id_type=MESH))
    copies = [pltpu.make_async_copy(tables_hbm, tables_ref, local_sems.at[4])] + [
        pltpu.make_async_copy(top_hbm.at[:, pl.ds(at * 128, 128)], raw_ref.at[at], local_sems.at[at])
        for at in range(4)
    ]
    for copy in copies:
        copy.start()

    prep_ids(rows_ref, lens_ref, counts_ref, ids_out)
    ids_in[me] = ids_out[me]
    pl.semaphore_wait(barrier, n - 1)

    def id_copy(src, dst, to):
        return pltpu.make_async_remote_copy(
            src_ref=src, dst_ref=dst, send_sem=ids_sems.at[0], recv_sem=ids_sems.at[1],
            device_id={"dev": to}, device_id_type=MESH,
        )

    each_other(lambda to: id_copy(ids_out.at[to], ids_in.at[me], to).start())
    copies[0].wait()
    pool_turn(tables_ref, turned_ref)
    for copy in copies[1:]:
        copy.wait()

    everyone = id_copy(ids_out.at[pl.ds(0, n - 1)], ids_in.at[pl.ds(0, n - 1)], (me + 1) % n)
    everyone.wait_recv()
    ids_wide[...] = ids_in[...].astype(I32)
    pool_setup(
        lambda q, j: ids_wide[pl.ds(q, 32, stride=4), j, :], y_ref, code_ref, pos_ref, scale_ref
    )

    def row_copy(src, dst, to, chunk):
        return pltpu.make_async_remote_copy(
            src_ref=src, dst_ref=dst, send_sem=send_sem.at[0], recv_sem=recv_sems.at[chunk],
            device_id={"dev": to}, device_id_type=MESH,
        )

    def block(ref, device):
        return ref.at[pl.ds(pl.multiple_of(device * ROOM, ROOM), ROOM), :]

    def step(t, carry):
        group = target(t)
        for j in range(4):
            pool_table(group, j, turned_ref, y_ref, code_ref, scale_ref, xt_ref)
        blocks = pool_pack(group, pos_ref, xt_ref)
        for half in range(2):
            send_ref[pl.ds(pl.multiple_of((2 * group + half) * 4 * ROOM, 4 * ROOM), 4 * ROOM), :] = blocks[half]
        for u in range(2):
            weight_cut(2 * t + u, raw_ref, plane_ref)

        def one(i, inner):
            to = group * 8 + (my_place + i) % 8

            @pl.when(to != me)
            def _():
                row_copy(block(send_ref, to), block(recv_ref, me), to, my_chunk).start()

            return inner

        lax.fori_loop(0, 8, one, 0)
        return carry

    lax.fori_loop(0, GROUPS, step, 0)
    target_setup(inverse_ref, counts_ref, order_ref, compress_ref, turn_ref, mix_ref)
    perm_ref[...] = order_columns(order_ref).astype(F32).T.astype(BF)
    for g in range(GROUPS):
        cols_ref[g] = mix_ref[:, g * 32 : g * 32 + 32]

    def clear(g, carry):
        rows = pl.ds(pl.multiple_of(arrived(GROUPS - 4 + g) * 32, 32), 32)
        feat_ref[:, :, rows, :] = jnp.zeros((64, 2, 32, 128), BF)
        return carry

    def arrived(u):
        return 2 * ((my_z + 8 - shift(u)) % 8) + (my_y + u) % 2

    lax.fori_loop(0, 4, clear, 0)
    mine = pl.ds(pl.multiple_of(me * ROOM, ROOM), ROOM)
    recv_ref[mine, :] = send_ref[mine, :]

    def take(u, carry):
        group = arrived(u)

        def half(v, inner):
            chunk = 2 * group + (my_chunk + v) % 2

            @pl.when(chunk == my_chunk)
            def _():
                rows = pl.ds(0, 3 * ROOM)
                row_copy(send_ref.at[rows, :], recv_ref.at[rows, :], (me + 1) % n, chunk).wait_recv()

            @pl.when(chunk != my_chunk)
            def _():
                rows = pl.ds(0, 4 * ROOM)
                row_copy(send_ref.at[rows, :], recv_ref.at[rows, :], (me + 1) % n, chunk).wait_recv()

            pick_chunk(chunk, recv_ref, turn_ref, feat_ref)
            return inner

        return lax.fori_loop(0, 2, half, carry)

    def turn_and_take(u, carry):
        for k in range(2):
            weight_plane(2 * u + k, perm_ref, plane_ref, raw_ref)
        return take(u, carry)

    lax.fori_loop(0, 8, turn_and_take, 0)
    lax.fori_loop(8, GROUPS - 4, take, 0)

    def keep(i, value):
        sum_ref[i] = value

    mixing(mix_ref[...], lambda i, v: feat_ref[i, v], keep)
    lax.fori_loop(GROUPS - 4, GROUPS, take, 0)
    last = [arrived(GROUPS - 4 + g) for g in range(4)]
    zero = jnp.zeros((16, 128), BF)

    def settle(i, value):
        mixed = (sum_ref[i] + value).astype(BF)
        for v in range(2):
            left_ref[i, v, v * 16 : v * 16 + 16, :] = mixed[:, v * 128 : v * 128 + 128]
            left_ref[i, v, 16 - v * 16 : 32 - v * 16, :] = zero

    mixing(
        jnp.concatenate([cols_ref[g] for g in last], axis=1),
        lambda i, v: jnp.concatenate(
            [feat_ref[i, v, pl.ds(pl.multiple_of(g * 32, 32), 32), :] for g in last], axis=0
        ),
        settle,
    )
    finish(
        feat_ref, lambda k, at: raw_ref[at, pl.ds(pl.multiple_of(k * 512, 512), 512), :],
        bias_ref, out_ref, left_ref, pair_ref, acc_ref,
    )
    everyone.wait_send()
    rows = pl.ds(0, (n - 1) * ROOM)
    row_copy(send_ref.at[rows, :], recv_ref.at[rows, :], (me + 1) % n, my_chunk).wait_send()


def shards(tables, bag_rows, bag_lengths, row_counts, inverse, table_order, compress, top_weight, top_bias):
    order = table_order.reshape(1, -1)
    bias = top_bias.reshape(1, -1)
    rows = bag_rows[0].transpose(1, 2, 0)
    lens = bag_lengths[0].transpose(1, 0)
    samples, units = inverse.shape[0], top_weight.shape[1]
    anywhere = pl.BlockSpec(memory_space=pl.ANY)
    scratch = (
        [pltpu.VMEM(tables.shape, BF)]
        + pool_scratch()
        + [
            pltpu.VMEM((units // 128, top_weight.shape[0], 128), BF),
            pltpu.VMEM((16, units // 128, 512, 128), BF),
            pltpu.VMEM((512, 512), BF),
            pltpu.VMEM((128, 4, 128), jnp.int16),
            pltpu.VMEM((128, 4, 128), jnp.int16),
            pltpu.VMEM((128, 4, 128), I32),
            pltpu.VMEM((128 * ROOM, 128), BF),
            pltpu.VMEM((128 * ROOM, 128), BF),
        ]
        + score_scratch()
        + [pltpu.VMEM((GROUPS, 16, 32), BF)]
        + [
            pltpu.SemaphoreType.DMA((5,)),
            pltpu.SemaphoreType.DMA((2,)),
            pltpu.SemaphoreType.DMA((1,)),
            pltpu.SemaphoreType.DMA((2 * GROUPS,)),
        ]
    )
    hidden = pl.pallas_call(
        lookup_body,
        out_shape=jax.ShapeDtypeStruct((samples, units), F32),
        in_specs=[VM] * 7 + [anywhere] * 2,
        out_specs=VM,
        scratch_shapes=scratch,
        compiler_params=pltpu.CompilerParams(vmem_limit_bytes=BIG, collective_id=0, has_side_effects=True),
        cost_estimate=pl.CostEstimate(flops=3 * 10**10, bytes_accessed=16 << 20, transcendentals=0),
    )(rows, lens, row_counts, inverse, order, compress, bias, tables, top_weight)
    return jnp.maximum(hidden, 0.0).astype(BF)


def solution(mesh):
    return jax.shard_map(
        shards,
        mesh=mesh,
        in_specs=(
            P("dev", None, None),
            P(("rep", "dev"), None, None, None),
            P(("rep", "dev"), None, None),
            P(("rep", "dev"), None),
            P(("rep", "dev"), None),
            P(),
            P(),
            P(),
            P(),
        ),
        out_specs=P(("rep", "dev"), None),
        check_vma=False,
    )
```

```python
import functools
import jax
import jax.numpy as jnp
from jax import lax
from jax.experimental import pallas as pl
from jax.experimental.pallas import tpu as pltpu
from jax.sharding import PartitionSpec as P

BF = jnp.bfloat16
F32 = jnp.float32
I32 = jnp.int32
ROOM = 80


def iota(shape, axis):
    return lax.broadcasted_iota(I32, shape, axis)


def onehot(mask):
    return jnp.where(mask, 1.0, 0.0).astype(BF)


def prep_ids(rows_ref, lens_ref, counts_ref, ids_out):
    most, pool, slots = rows_ref.shape
    used = iota((most, slots), 0) < counts_ref[...]
    lens = lens_ref[...]
    wide = jnp.concatenate(
        [jnp.where(used & (p < lens), rows_ref[:, p, :], -1) for p in range(pool)], axis=0
    )
    for at in range(slots // 128):
        turned = wide[:, at * 128 : (at + 1) * 128].T.reshape(32, 4, 128)
        ids_out[at * 32 : at * 32 + 32] = turned.astype(jnp.int16)


PLANE = 128


def pool_turn(tables_ref, turned_ref):
    tabs, vocab, width = tables_ref.shape
    for j in range(tabs):
        for at in range(vocab // 128):
            turned_ref[j, at] = (
                tables_ref[j, at * 128 : at * 128 + 128, :].astype(F32).T * (0.25 ** (at % 4))
            ).astype(BF)


def pool_setup(load_ids, y_ref, code_ref, pos_ref, scale_ref):
    lane = iota((2, 128), 1)
    chunk = lane // 32
    same = onehot(iota((128, 128), 0) // 32 == iota((128, 128), 1) // 32)
    base = jnp.zeros((2, 128), F32)
    for j in range(4):
        got = [load_ids(q, j) for q in range(4)]
        ys = []
        for p in range(4):
            y = got[0] if p == 0 else pltpu.roll(got[0], (-p * 32) % 128, 1)
            for q in range(1, 4):
                moved = got[q] if p == q else pltpu.roll(got[q], ((q - p) * 32) % 128, 1)
                y = jnp.where(chunk == q, moved, y)
            ys.append(y)
        valid = ys[0] >= 0
        total = jnp.dot(onehot(valid), same, preferred_element_type=F32)
        place = base.astype(I32) + (lane % 32) + chunk * ROOM
        pos_ref[j * 8 : j * 8 + 2, :] = jnp.where(valid, place, -1)
        base = base + total
        alike = (ys[0] == ys[1]) & (ys[0] == ys[2]) & (ys[0] == ys[3])
        scale_ref[j * 8 : j * 8 + 2, :] = jnp.where(alike, 2.0, 1.0)
        for p in range(4):
            y = ys[p]
            live = (y >= 0) if p < 2 else ((y >= 0) & ~alike)
            code = jnp.where(live, jnp.left_shift(jnp.ones_like(y), ((y >> 7) * 2) & 31), 0)
            at = (j * 4 + p) * 8
            y_ref[at : at + 2, :] = y & 127
            for k in range(4):
                code_ref[k * PLANE + at : k * PLANE + at + 2, :] = (
                    lax.shift_right_logical(code, jnp.full_like(code, 8 * k)) & 255
                )


def small(ref, at):
    return jnp.broadcast_to(ref[pl.ds(at, 1), :], (16, 128)).astype(jnp.int16)


def pool_table(j, turned_ref, y_ref, code_ref, scale_ref, xt_ref):
    low_iota = iota((16, 128), 0).astype(jnp.int16)
    zero = jnp.zeros((16, 128), jnp.int16)
    rows = [[(j * 4 + p) * 8 + half for p in range(4)] for half in range(2)]
    hits = []
    for half in range(2):
        lows = [small(y_ref, row) for row in rows[half]]
        hits.append([[low == low_iota + jnp.int16(16 * at) for low in lows] for at in range(8)])
    total = None
    for k in range(4):
        planes = []
        for half in range(2):
            codes = [small(code_ref, k * PLANE + row) for row in rows[half]]
            plane = []
            for hit in hits[half]:
                cut = [jnp.where(hit[p], codes[p], zero) for p in range(4)]
                plane.append((cut[0] + cut[1]) + (cut[2] + cut[3]))
            planes.append(jnp.concatenate(plane, axis=0).astype(jnp.uint8))
        for i in (0, 2):
            hot = jnp.concatenate(
                [
                    jnp.concatenate([(plane & jnp.uint8(3 << (2 * u))).astype(BF) for u in (i, i + 1)], axis=0)
                    for plane in planes
                ],
                axis=1,
            )
            left = jnp.concatenate([turned_ref[j, 4 * k + i], turned_ref[j, 4 * k + i + 1]], axis=1)
            part = jnp.dot(left, hot, preferred_element_type=F32)
            total = part if total is None else total + part
    for half in range(2):
        scale = scale_ref[pl.ds(j * 8 + half, 1), :]
        xt_ref[half, j] = (total[:, half * 128 : half * 128 + 128] * scale).astype(BF)


def pool_pack(pos_ref, xt_ref):
    out = []
    for half in range(2):
        total = None
        for jj in range(2):
            packs, cols = [], []
            for j in (2 * jj, 2 * jj + 1):
                pos = small(pos_ref, j * 8 + half)
                hits = [
                    jnp.where(
                        pos == iota((16, 128), 0).astype(jnp.int16) + jnp.int16(16 * at),
                        jnp.ones((16, 128), BF),
                        jnp.zeros((16, 128), BF),
                    )
                    for at in range(4 * ROOM // 16)
                ]
                packs.append(jnp.concatenate(hits, axis=0))
                cols.append(xt_ref[half, j])
            part = lax.dot_general(
                jnp.concatenate(packs, axis=1),
                jnp.concatenate(cols, axis=1),
                (((1,), (1,)), ((), ())),
                preferred_element_type=F32,
            )
            total = part if total is None else total + part
        out.append(total.astype(BF))
    return out


def pool_scratch():
    return [
        pltpu.VMEM((4, 16, 128, 128), BF),
        pltpu.VMEM((PLANE, 128), I32),
        pltpu.VMEM((4 * PLANE, 128), I32),
        pltpu.VMEM((32, 128), I32),
        pltpu.VMEM((32, 128), F32),
        pltpu.VMEM((2, 4, 128, 128), BF),
    ]


def order_columns(order_ref):
    slots = order_ref.shape[1]
    return onehot(iota((slots, slots), 0) == order_ref[...])


def weight_cut(at, raw_ref, plane_ref):
    row = iota((256, 256), 0)
    col = iota((256, 256), 1)
    spread = onehot((col % 16 == row // 16) & (col // 16 == row % 16))
    rows = pl.ds(pl.multiple_of(at * 256, 256), 256)
    block = jnp.dot(
        spread, jnp.concatenate([raw_ref[c, rows, :] for c in range(4)], axis=1), preferred_element_type=F32
    ).astype(BF)
    for k in range(16):
        for c in range(4):
            plane_ref[k, c, pl.ds(pl.multiple_of(at * 16, 16), 16), :] = block[
                k * 16 : k * 16 + 16, c * 128 : c * 128 + 128
            ]


def weight_plane(k, perm_ref, plane_ref, raw_ref):
    plane = jnp.concatenate([plane_ref[k, c] for c in range(4)], axis=1)
    done = jnp.dot(perm_ref[...], plane, preferred_element_type=F32).astype(BF)
    for c in range(4):
        raw_ref[c, pl.ds(pl.multiple_of(k * 512, 512), 512), :] = done[:, c * 128 : c * 128 + 128]


def target_setup(inverse_ref, counts_ref, order_ref, compress_ref, turn_ref, mix_ref):
    samples, slots = inverse_ref.shape
    columns = order_columns(order_ref)
    mix_ref[...] = jnp.dot(compress_ref[...], columns, preferred_element_type=F32).astype(BF)
    chosen = jnp.dot(inverse_ref[...].astype(F32).astype(BF), columns, preferred_element_type=F32)
    counts = jnp.broadcast_to(counts_ref[...], (16, slots)).astype(F32)
    before = (iota((slots, slots), 0) // 4 == iota((slots, slots), 1) // 4) & (
        iota((slots, slots), 0) < iota((slots, slots), 1)
    )
    base = jnp.dot(counts.astype(BF), onehot(before), preferred_element_type=F32)[:1, :]
    offset = ((iota((1, slots), 1) // 4) % 2 * ROOM).astype(F32)
    place = jnp.where(chosen < counts[:1, :], chosen + (base + offset), 255.0)
    for at in range(slots // 128):
        turned = place[:, at * 128 : (at + 1) * 128].T.astype(I32).reshape(8, 16, 128)
        upper, lower = turned[:, :8].reshape(64, 128), turned[:, 8:].reshape(64, 128)
        two = upper | (lower << 8)
        turn_ref[pl.ds(at * 64, 64), :] = two | (pltpu.roll(two, 64, 1) << 16)


def pick_chunk(c, packed_ref, turn_ref, feat_ref):
    place = turn_ref[pl.ds(pl.multiple_of(c * 8, 8), 8), :]
    near = iota((16, 128), 1).astype(jnp.int16)
    far = near + jnp.int16(128)
    one, zero = jnp.ones((16, 128), BF), jnp.zeros((16, 128), BF)
    rows = jnp.concatenate(
        [packed_ref[pl.ds(pl.multiple_of(c * 320 + h * 160, 160), 160), :] for h in range(2)], axis=1
    )
    at = pl.ds(pl.multiple_of(c * 16, 16), 16)
    for part in range(4):
        left, right = [[], []], [[], []]
        for b in range(part * 16, part * 16 + 16):
            x = jnp.broadcast_to(place[:, b : b + 1], (8, 128))
            for v in range(2):
                cut = [(x >> (16 * v)) & 255, (x >> (16 * v + 8)) & 255]
                want = jnp.concatenate(cut, axis=0).astype(jnp.int16)
                left[v].append(jnp.where(want == near, one, zero))
                right[v].append(jnp.where(want == far, one, zero)[:, :32])
        got = jnp.dot(
            jnp.concatenate(
                [jnp.concatenate(left[0] + left[1], axis=0), jnp.concatenate(right[0] + right[1], axis=0)], axis=1
            ),
            rows,
            preferred_element_type=F32,
        ).reshape(2, 16, 16, 256)
        both = jnp.concatenate([got[:, :, :8, :128], got[:, :, 8:, 128:]], axis=2).astype(BF)
        for v in range(2):
            feat_ref[part * 16 : part * 16 + 16, v, at, :] = both[v]


def mixing(columns, feats_of, store):
    def some(i, carry):
        for u in range(16):
            feats = jnp.concatenate([feats_of(i * 16 + u, v) for v in range(2)], axis=1)
            store(i * 16 + u, jnp.dot(columns, feats, preferred_element_type=F32))
        return carry

    lax.fori_loop(0, 4, some, 0)


def finish(feat_ref, weight_at, bias_ref, out_ref, left_ref, pair_ref, acc_ref):
    def pairing(i, carry):
        for u in range(16):
            sides = [
                jnp.concatenate([ref[i * 16 + u, v] for v in range(2)], axis=1) for ref in (left_ref, feat_ref)
            ]
            both = lax.dot_general(
                sides[0], sides[1], (((1,), (1,)), ((), ())), preferred_element_type=F32
            )
            for v in range(2):
                to = pl.ds(pl.multiple_of((v * 64 + i * 16 + u) * 24, 8), 16)
                for at in range(4):
                    pair_ref[at, to, :] = both[v * 16 : v * 16 + 16, at * 128 : at * 128 + 128]
        return carry

    lax.fori_loop(0, 4, pairing, 0)
    acc_ref[...] = jnp.broadcast_to(bias_ref[...], acc_ref.shape)

    def plane(i, carry):
        total = acc_ref[...]
        for u in range(8):
            k = i * 8 + u
            lhs = jnp.concatenate(
                [pair_ref[at, pl.ds(k, 128, stride=24), :].astype(BF) for at in range(4)], axis=1
            )
            total = total + jnp.dot(
                lhs, jnp.concatenate([weight_at(k, at) for at in range(4)], axis=1), preferred_element_type=F32)
        acc_ref[...] = total
        return carry

    lax.fori_loop(0, 2, plane, 0)
    out_ref[...] = acc_ref[...]


def score_scratch():
    return [
        pltpu.VMEM((256, 128), I32),
        pltpu.VMEM((16, 512), BF),
        pltpu.VMEM((64, 2, 512, 128), BF),
        pltpu.VMEM((64, 2, 32, 128), BF),
        pltpu.VMEM((64, 16, 256), F32),
        pltpu.VMEM((4, 3072, 128), F32),
        pltpu.VMEM((128, 512), F32),
    ]


VM = pl.BlockSpec(memory_space=pltpu.VMEM)
BIG = 56 * 1024 * 1024


MESH = pl.DeviceIdType.MESH
GROUPS = 16
ORDER = [(1, 0), (7, 0), (1, 1), (7, 1), (4, 0), (4, 1), (3, 0), (5, 0)]
ORDER += [(3, 1), (5, 1), (0, 0), (0, 1), (2, 0), (6, 0), (2, 1), (6, 1)]
SHIFTS = [sum(ORDER[8 * part + at][0] << (3 * at) for at in range(8)) for part in range(2)]
HALVES = sum(dy << at for at, (_, dy) in enumerate(ORDER))


def lookup_body(
    rows_ref, lens_ref, counts_ref, inverse_ref, order_ref, compress_ref, bias_ref, tables_hbm, top_hbm,
    out_ref,
    tables_ref, turned_ref, y_ref, code_ref, pos_ref, scale_ref, xt_ref,
    raw_ref, plane_ref, perm_ref, ids_out, ids_in, ids_wide, send_ref, recv_ref,
    turn_ref, mix_ref, feat_ref, left_ref, sum_ref, pair_ref, acc_ref, cols_ref,
    local_sems, ids_sems, send_sem, recv_sems,
):
    n = 8 * GROUPS
    me = lax.axis_index("dev")
    my_group, my_place, my_chunk = me // 8, me % 8, me // 4
    my_z, my_y = my_group // 2, my_group % 2

    def turn_of(t):
        shifts = jnp.where(t < 8, SHIFTS[0], SHIFTS[1])
        return (shifts >> (3 * (t & 7))) & 7, (HALVES >> t) & 1

    def target(t):
        dz, dy = turn_of(t)
        return 2 * ((my_z + dz) & 7) + ((my_y + dy) & 1)

    def each_other(act):
        def some(t, carry):
            for i in range(8):
                act((me + n // 2 + t * 8 + i) & (n - 1))
            return carry

        lax.fori_loop(0, n // 16, some, 0)
        for i in range(1, 8):
            act((me + i) & (n - 1))
        lax.fori_loop(n // 16 + 1, n // 8, some, 0)

    barrier = pltpu.get_barrier_semaphore()
    each_other(lambda to: pl.semaphore_signal(barrier, 1, device_id={"dev": to}, device_id_type=MESH))
    copies = [pltpu.make_async_copy(tables_hbm, tables_ref, local_sems.at[4])] + [
        pltpu.make_async_copy(top_hbm.at[:, pl.ds(at * 128, 128)], raw_ref.at[at], local_sems.at[at])
        for at in range(4)
    ]
    for copy in copies:
        copy.start()

    prep_ids(rows_ref, lens_ref, counts_ref, ids_out)
    ids_in[me] = ids_out[me]
    pl.semaphore_wait(barrier, n - 1)

    def id_copy(src, dst, to, group):
        return pltpu.make_async_remote_copy(
            src_ref=src, dst_ref=dst, send_sem=send_sem.at[1], recv_sem=ids_sems.at[group],
            device_id={"dev": to}, device_id_type=MESH,
        )

    each_other(lambda to: id_copy(ids_out.at[to], ids_in.at[me], to, my_group).start())
    copies[0].wait()
    pool_turn(tables_ref, turned_ref)
    for copy in copies[1:]:
        copy.wait()

    def ids_of(group, count):
        some = pl.ds(0, count)
        return id_copy(ids_out.at[some], ids_in.at[some], (me + 1) % n, group)

    def row_copy(src, dst, to, chunk):
        return pltpu.make_async_remote_copy(
            src_ref=src, dst_ref=dst, send_sem=send_sem.at[0], recv_sem=recv_sems.at[chunk],
            device_id={"dev": to}, device_id_type=MESH,
        )

    def block(ref, device):
        return ref.at[pl.ds(pl.multiple_of(device * ROOM, ROOM), ROOM), :]

    def step(t, carry):
        group = target(t)

        @pl.when(group == my_group)
        def _():
            ids_of(group, 7).wait_recv()

        @pl.when(group != my_group)
        def _():
            ids_of(group, 8).wait_recv()

        ids_wide[...] = ids_in[pl.ds(pl.multiple_of(group * 8, 8), 8)].astype(I32)
        pool_setup(
            lambda q, j: ids_wide[pl.ds(q, 2, stride=4), j, :], y_ref, code_ref, pos_ref, scale_ref
        )
        for j in range(4):
            pool_table(j, turned_ref, y_ref, code_ref, scale_ref, xt_ref)
        blocks = pool_pack(pos_ref, xt_ref)
        for half in range(2):
            send_ref[pl.ds(pl.multiple_of((2 * group + half) * 4 * ROOM, 4 * ROOM), 4 * ROOM), :] = blocks[half]
        for u in range(2):
            weight_cut(2 * t + u, raw_ref, plane_ref)

        def one(i, inner):
            to = group * 8 + (my_place + i) % 8

            @pl.when(to != me)
            def _():
                row_copy(block(send_ref, to), block(recv_ref, me), to, my_chunk).start()

            return inner

        lax.fori_loop(0, 8, one, 0)
        return carry

    lax.fori_loop(0, GROUPS, step, 0)
    target_setup(inverse_ref, counts_ref, order_ref, compress_ref, turn_ref, mix_ref)
    perm_ref[...] = order_columns(order_ref).astype(F32).T.astype(BF)
    for g in range(GROUPS):
        cols_ref[g] = mix_ref[:, g * 32 : g * 32 + 32]

    def clear(g, carry):
        rows = pl.ds(pl.multiple_of(arrived(GROUPS - 4 + g) * 32, 32), 32)
        feat_ref[:, :, rows, :] = jnp.zeros((64, 2, 32, 128), BF)
        return carry

    def arrived(u):
        dz, dy = turn_of(u)
        return 2 * ((my_z + 8 - dz) & 7) + ((my_y + dy) & 1)

    lax.fori_loop(0, 4, clear, 0)
    mine = pl.ds(pl.multiple_of(me * ROOM, ROOM), ROOM)
    recv_ref[mine, :] = send_ref[mine, :]

    def take(u, v):
        chunk = 2 * arrived(u) + (my_chunk + v) % 2

        @pl.when(chunk == my_chunk)
        def _():
            rows = pl.ds(0, 3 * ROOM)
            row_copy(send_ref.at[rows, :], recv_ref.at[rows, :], (me + 1) % n, chunk).wait_recv()

        @pl.when(chunk != my_chunk)
        def _():
            rows = pl.ds(0, 4 * ROOM)
            row_copy(send_ref.at[rows, :], recv_ref.at[rows, :], (me + 1) % n, chunk).wait_recv()

        pick_chunk(chunk, recv_ref, turn_ref, feat_ref)

    def turn_and_take(w, carry):
        weight_plane(w, perm_ref, plane_ref, raw_ref)
        take(w // 2, w % 2)
        return carry

    def only_take(w, carry):
        take(w // 2, w % 2)
        return carry

    def last_take(w, carry):
        late = w // 4
        take(
            GROUPS - 4 + 2 * late + jnp.where(late == 1, w % 2, w // 2),
            jnp.where(late == 1, (w - 4) // 2, w % 2),
        )
        return carry

    lax.fori_loop(0, 16, turn_and_take, 0)
    lax.fori_loop(16, 2 * GROUPS - 8, only_take, 0)

    def keep(i, value):
        sum_ref[i] = value

    mixing(mix_ref[...], lambda i, v: feat_ref[i, v], keep)
    lax.fori_loop(0, 8, last_take, 0)
    last = [arrived(GROUPS - 4 + g) for g in range(4)]
    zero = jnp.zeros((16, 128), BF)

    def settle(i, value):
        mixed = (sum_ref[i] + value).astype(BF)
        for v in range(2):
            left_ref[i, v, v * 16 : v * 16 + 16, :] = mixed[:, v * 128 : v * 128 + 128]
            left_ref[i, v, 16 - v * 16 : 32 - v * 16, :] = zero

    mixing(
        jnp.concatenate([cols_ref[g] for g in last], axis=1),
        lambda i, v: jnp.concatenate(
            [feat_ref[i, v, pl.ds(pl.multiple_of(g * 32, 32), 32), :] for g in last], axis=0
        ),
        settle,
    )
    finish(
        feat_ref, lambda k, at: raw_ref[at, pl.ds(pl.multiple_of(k * 512, 512), 512), :],
        bias_ref, out_ref, left_ref, pair_ref, acc_ref,
    )
    ids_of(my_group, n - 1).wait_send()
    rows = pl.ds(0, (n - 1) * ROOM)
    row_copy(send_ref.at[rows, :], recv_ref.at[rows, :], (me + 1) % n, my_chunk).wait_send()


def shards(tables, bag_rows, bag_lengths, row_counts, inverse, table_order, compress, top_weight, top_bias):
    order = table_order.reshape(1, -1)
    bias = top_bias.reshape(1, -1)
    rows = bag_rows[0].transpose(1, 2, 0)
    lens = bag_lengths[0].transpose(1, 0)
    samples, units = inverse.shape[0], top_weight.shape[1]
    anywhere = pl.BlockSpec(memory_space=pl.ANY)
    scratch = (
        [pltpu.VMEM(tables.shape, BF)]
        + pool_scratch()
        + [
            pltpu.VMEM((units // 128, top_weight.shape[0], 128), BF),
            pltpu.VMEM((16, units // 128, 512, 128), BF),
            pltpu.VMEM((512, 512), BF),
            pltpu.VMEM((128, 4, 128), jnp.int16),
            pltpu.VMEM((128, 4, 128), jnp.int16),
            pltpu.VMEM((8, 4, 128), I32),
            pltpu.VMEM((128 * ROOM, 128), BF),
            pltpu.VMEM((128 * ROOM, 128), BF),
        ]
        + score_scratch()
        + [pltpu.VMEM((GROUPS, 16, 32), BF)]
        + [
            pltpu.SemaphoreType.DMA((5,)),
            pltpu.SemaphoreType.DMA((GROUPS,)),
            pltpu.SemaphoreType.DMA((2,)),
            pltpu.SemaphoreType.DMA((2 * GROUPS,)),
        ]
    )
    hidden = pl.pallas_call(
        lookup_body,
        out_shape=jax.ShapeDtypeStruct((samples, units), F32),
        in_specs=[VM] * 7 + [anywhere] * 2,
        out_specs=VM,
        scratch_shapes=scratch,
        compiler_params=pltpu.CompilerParams(vmem_limit_bytes=BIG, collective_id=0, has_side_effects=True),
        cost_estimate=pl.CostEstimate(flops=3 * 10**10, bytes_accessed=16 << 20, transcendentals=0),
    )(rows, lens, row_counts, inverse, order, compress, bias, tables, top_weight)
    return jnp.maximum(hidden, 0.0).astype(BF)


def solution(mesh):
    return jax.shard_map(
        shards,
        mesh=mesh,
        in_specs=(
            P("dev", None, None),
            P(("rep", "dev"), None, None, None),
            P(("rep", "dev"), None, None),
            P(("rep", "dev"), None),
            P(("rep", "dev"), None),
            P(),
            P(),
            P(),
            P(),
        ),
        out_specs=P(("rep", "dev"), None),
        check_vma=False,
    )
```

```python
import functools
import jax
import jax.numpy as jnp
from jax import lax
from jax.experimental import pallas as pl
from jax.experimental.pallas import tpu as pltpu
from jax.sharding import PartitionSpec as P

BF = jnp.bfloat16
F32 = jnp.float32
I32 = jnp.int32
ROOM = 80


def iota(shape, axis):
    return lax.broadcasted_iota(I32, shape, axis)


def onehot(mask):
    return jnp.where(mask, 1.0, 0.0).astype(BF)


def prep_ids(rows_ref, lens_ref, counts_ref, ids_out):
    most, pool, slots = rows_ref.shape
    used = iota((most, slots), 0) < counts_ref[...]
    lens = lens_ref[...]
    wide = jnp.concatenate(
        [jnp.where(used & (p < lens), rows_ref[:, p, :], -1) for p in range(pool)], axis=0
    )
    for at in range(slots // 128):
        turned = wide[:, at * 128 : (at + 1) * 128].T.reshape(32, 4, 128)
        ids_out[at * 32 : at * 32 + 32] = turned.astype(jnp.int16)


PLANE = 128


def pool_turn(tables_ref, turned_ref):
    tabs, vocab, width = tables_ref.shape
    for j in range(tabs):
        for at in range(vocab // 128):
            turned_ref[j, at] = (
                tables_ref[j, at * 128 : at * 128 + 128, :].astype(F32).T * (0.25 ** (at % 4))
            ).astype(BF)


def pool_setup(load_ids, y_ref, code_ref, pos_ref, scale_ref):
    lane = iota((2, 128), 1)
    chunk = lane // 32
    same = onehot(iota((128, 128), 0) // 32 == iota((128, 128), 1) // 32)
    base = jnp.zeros((2, 128), F32)
    for j in range(4):
        got = [load_ids(q, j) for q in range(4)]
        ys = []
        for p in range(4):
            y = got[0] if p == 0 else pltpu.roll(got[0], (-p * 32) % 128, 1)
            for q in range(1, 4):
                moved = got[q] if p == q else pltpu.roll(got[q], ((q - p) * 32) % 128, 1)
                y = jnp.where(chunk == q, moved, y)
            ys.append(y)
        valid = ys[0] >= 0
        total = jnp.dot(onehot(valid), same, preferred_element_type=F32)
        place = base.astype(I32) + (lane % 32) + chunk * ROOM
        pos_ref[j * 8 : j * 8 + 2, :] = jnp.where(valid, place, -1)
        base = base + total
        alike = (ys[0] == ys[1]) & (ys[0] == ys[2]) & (ys[0] == ys[3])
        scale_ref[j * 8 : j * 8 + 2, :] = jnp.where(alike, 2.0, 1.0)
        for p in range(4):
            y = ys[p]
            live = (y >= 0) if p < 2 else ((y >= 0) & ~alike)
            code = jnp.where(live, jnp.left_shift(jnp.ones_like(y), ((y >> 7) * 2) & 31), 0)
            at = (j * 4 + p) * 8
            y_ref[at : at + 2, :] = y & 127
            for k in range(4):
                code_ref[k * PLANE + at : k * PLANE + at + 2, :] = (
                    lax.shift_right_logical(code, jnp.full_like(code, 8 * k)) & 255
                )


def small(ref, at):
    return jnp.broadcast_to(ref[pl.ds(at, 1), :], (16, 128)).astype(jnp.int16)


def pool_table(j, turned_ref, y_ref, code_ref, scale_ref, xt_ref):
    low_iota = iota((16, 128), 0).astype(jnp.int16)
    zero = jnp.zeros((16, 128), jnp.int16)
    rows = [[(j * 4 + p) * 8 + half for p in range(4)] for half in range(2)]
    hits = []
    for half in range(2):
        lows = [small(y_ref, row) for row in rows[half]]
        hits.append([[low == low_iota + jnp.int16(16 * at) for low in lows] for at in range(8)])
    total = None
    for k in range(4):
        planes = []
        for half in range(2):
            codes = [small(code_ref, k * PLANE + row) for row in rows[half]]
            plane = []
            for hit in hits[half]:
                cut = [jnp.where(hit[p], codes[p], zero) for p in range(4)]
                plane.append((cut[0] + cut[1]) + (cut[2] + cut[3]))
            planes.append(jnp.concatenate(plane, axis=0).astype(jnp.uint8))
        for i in (0, 2):
            hot = jnp.concatenate(
                [
                    jnp.concatenate([(plane & jnp.uint8(3 << (2 * u))).astype(BF) for u in (i, i + 1)], axis=0)
                    for plane in planes
                ],
                axis=1,
            )
            left = jnp.concatenate([turned_ref[j, 4 * k + i], turned_ref[j, 4 * k + i + 1]], axis=1)
            part = jnp.dot(left, hot, preferred_element_type=F32)
            total = part if total is None else total + part
    for half in range(2):
        scale = scale_ref[pl.ds(j * 8 + half, 1), :]
        xt_ref[half, j] = (total[:, half * 128 : half * 128 + 128] * scale).astype(BF)


def pool_pack(pos_ref, xt_ref):
    out = []
    for half in range(2):
        total = None
        for jj in range(2):
            packs, cols = [], []
            for j in (2 * jj, 2 * jj + 1):
                pos = small(pos_ref, j * 8 + half)
                hits = [
                    jnp.where(
                        pos == iota((16, 128), 0).astype(jnp.int16) + jnp.int16(16 * at),
                        jnp.ones((16, 128), BF),
                        jnp.zeros((16, 128), BF),
                    )
                    for at in range(4 * ROOM // 16)
                ]
                packs.append(jnp.concatenate(hits, axis=0))
                cols.append(xt_ref[half, j])
            part = lax.dot_general(
                jnp.concatenate(packs, axis=1),
                jnp.concatenate(cols, axis=1),
                (((1,), (1,)), ((), ())),
                preferred_element_type=F32,
            )
            total = part if total is None else total + part
        out.append(total.astype(BF))
    return out


def pool_scratch():
    return [
        pltpu.VMEM((4, 16, 128, 128), BF),
        pltpu.VMEM((PLANE, 128), I32),
        pltpu.VMEM((4 * PLANE, 128), I32),
        pltpu.VMEM((32, 128), I32),
        pltpu.VMEM((32, 128), F32),
        pltpu.VMEM((2, 4, 128, 128), BF),
    ]


def order_columns(order_ref):
    slots = order_ref.shape[1]
    return onehot(iota((slots, slots), 0) == order_ref[...])


def weight_cut(at, raw_ref, plane_ref):
    row = iota((256, 256), 0)
    col = iota((256, 256), 1)
    spread = onehot((col % 16 == row // 16) & (col // 16 == row % 16))
    rows = pl.ds(pl.multiple_of(at * 256, 256), 256)
    block = jnp.dot(
        spread, jnp.concatenate([raw_ref[c, rows, :] for c in range(4)], axis=1), preferred_element_type=F32
    ).astype(BF)
    for k in range(16):
        for c in range(4):
            plane_ref[k, c, pl.ds(pl.multiple_of(at * 16, 16), 16), :] = block[
                k * 16 : k * 16 + 16, c * 128 : c * 128 + 128
            ]


def weight_plane(k, perm_ref, plane_ref, raw_ref):
    plane = jnp.concatenate([plane_ref[k, c] for c in range(4)], axis=1)
    done = jnp.dot(perm_ref[...], plane, preferred_element_type=F32).astype(BF)
    for c in range(4):
        raw_ref[c, pl.ds(pl.multiple_of(k * 512, 512), 512), :] = done[:, c * 128 : c * 128 + 128]


def target_setup(inverse_ref, counts_ref, order_ref, compress_ref, turn_ref, mix_ref):
    samples, slots = inverse_ref.shape
    columns = order_columns(order_ref)
    mix_ref[...] = jnp.dot(compress_ref[...], columns, preferred_element_type=F32).astype(BF)
    chosen = jnp.dot(inverse_ref[...].astype(F32).astype(BF), columns, preferred_element_type=F32)
    counts = jnp.broadcast_to(counts_ref[...], (16, slots)).astype(F32)
    before = (iota((slots, slots), 0) // 4 == iota((slots, slots), 1) // 4) & (
        iota((slots, slots), 0) < iota((slots, slots), 1)
    )
    base = jnp.dot(counts.astype(BF), onehot(before), preferred_element_type=F32)[:1, :]
    offset = ((iota((1, slots), 1) // 4) % 2 * ROOM).astype(F32)
    place = jnp.where(chosen < counts[:1, :], chosen + (base + offset), 255.0)
    for at in range(slots // 128):
        turned = place[:, at * 128 : (at + 1) * 128].T.astype(I32).reshape(8, 16, 128)
        upper, lower = turned[:, :8].reshape(64, 128), turned[:, 8:].reshape(64, 128)
        two = upper | (lower << 8)
        turn_ref[pl.ds(at * 64, 64), :] = two | (pltpu.roll(two, 64, 1) << 16)


def pick_chunk(c, packed_ref, turn_ref, feat_ref):
    place = turn_ref[pl.ds(pl.multiple_of(c * 8, 8), 8), :]
    near = iota((16, 128), 1).astype(jnp.int16)
    far = near + jnp.int16(128)
    one, zero = jnp.ones((16, 128), BF), jnp.zeros((16, 128), BF)
    rows = jnp.concatenate(
        [packed_ref[pl.ds(pl.multiple_of(c * 320 + h * 160, 160), 160), :] for h in range(2)], axis=1
    )
    at = pl.ds(pl.multiple_of(c * 16, 16), 16)
    for part in range(4):
        left, right = [[], []], [[], []]
        for b in range(part * 16, part * 16 + 16):
            x = jnp.broadcast_to(place[:, b : b + 1], (8, 128))
            for v in range(2):
                cut = [(x >> (16 * v)) & 255, (x >> (16 * v + 8)) & 255]
                want = jnp.concatenate(cut, axis=0).astype(jnp.int16)
                left[v].append(jnp.where(want == near, one, zero))
                right[v].append(jnp.where(want == far, one, zero)[:, :32])
        got = jnp.dot(
            jnp.concatenate(
                [jnp.concatenate(left[0] + left[1], axis=0), jnp.concatenate(right[0] + right[1], axis=0)], axis=1
            ),
            rows,
            preferred_element_type=F32,
        ).reshape(2, 16, 16, 256)
        both = jnp.concatenate([got[:, :, :8, :128], got[:, :, 8:, 128:]], axis=2).astype(BF)
        for v in range(2):
            feat_ref[part * 16 : part * 16 + 16, v, at, :] = both[v]


def mixing(columns, feats_of, store):
    def some(i, carry):
        for u in range(16):
            feats = jnp.concatenate([feats_of(i * 16 + u, v) for v in range(2)], axis=1)
            store(i * 16 + u, jnp.dot(columns, feats, preferred_element_type=F32))
        return carry

    lax.fori_loop(0, 4, some, 0)


def finish(feat_ref, weight_at, bias_ref, out_ref, left_ref, pair_ref, acc_ref):
    def pairing(i, carry):
        for u in range(32):
            sides = [
                jnp.concatenate([ref[i * 32 + u, v] for v in range(2)], axis=1) for ref in (left_ref, feat_ref)
            ]
            both = lax.dot_general(
                sides[0], sides[1], (((1,), (1,)), ((), ())), preferred_element_type=F32
            )
            for v in range(2):
                to = pl.ds(pl.multiple_of((v * 64 + i * 32 + u) * 24, 8), 16)
                for at in range(4):
                    pair_ref[at, to, :] = both[v * 16 : v * 16 + 16, at * 128 : at * 128 + 128]
        return carry

    lax.fori_loop(0, 2, pairing, 0)
    acc_ref[...] = jnp.broadcast_to(bias_ref[...], acc_ref.shape)

    def plane(i, carry):
        total = acc_ref[...]
        for u in range(8):
            k = i * 8 + u
            lhs = jnp.concatenate(
                [pair_ref[at, pl.ds(k, 128, stride=24), :].astype(BF) for at in range(4)], axis=1
            )
            total = total + jnp.dot(
                lhs, jnp.concatenate([weight_at(k, at) for at in range(4)], axis=1), preferred_element_type=F32)
        acc_ref[...] = total
        return carry

    lax.fori_loop(0, 2, plane, 0)
    out_ref[...] = acc_ref[...]


def score_scratch():
    return [
        pltpu.VMEM((256, 128), I32),
        pltpu.VMEM((16, 512), BF),
        pltpu.VMEM((64, 2, 512, 128), BF),
        pltpu.VMEM((64, 2, 32, 128), BF),
        pltpu.VMEM((64, 16, 256), F32),
        pltpu.VMEM((4, 3072, 128), F32),
        pltpu.VMEM((128, 512), F32),
    ]


VM = pl.BlockSpec(memory_space=pltpu.VMEM)
BIG = 56 * 1024 * 1024


MESH = pl.DeviceIdType.MESH
GROUPS = 16
ORDER = [(1, 0), (1, 1)] + [(4, y) for y in range(4)] + [(3, y) for y in range(4)] + [(2, y) for y in range(4)]
ORDER += [(1, 2), (1, 3)]
SHIFTS = [sum(ORDER[8 * part + at][0] << (3 * at) for at in range(8)) for part in range(2)]
SIDES = sum(dy << (2 * at) for at, (_, dy) in enumerate(ORDER[:15]))
NEAR = [13, 14, 1, 2, 12, 15, 3, 4, 11, 5, 10, 6, 9, 7, 8]
NEARS = [sum(part[at] << (4 * at) for at in range(len(part))) for part in (NEAR[:7], NEAR[7:14])]


def lookup_body(
    rows_ref, lens_ref, counts_ref, inverse_ref, order_ref, compress_ref, bias_ref, tables_hbm, top_hbm,
    out_ref,
    tables_ref, turned_ref, y_ref, code_ref, pos_ref, scale_ref, xt_ref,
    raw_ref, plane_ref, perm_ref, ids_out, ids_in, ids_wide, send_ref, recv_ref,
    turn_ref, mix_ref, feat_ref, left_ref, sum_ref, pair_ref, acc_ref, cols_ref,
    local_sems, ids_sems, send_sem, recv_sems,
):
    n = 8 * GROUPS
    me = lax.axis_index("dev")
    my_place, my_chunk = me & 3, me // 4
    my_z, my_y = my_chunk // 4, my_chunk & 3

    def turn_of(t, half):
        dz = (jnp.where(t < 8, SHIFTS[0], SHIFTS[1]) >> (3 * (t & 7))) & 7
        dy = jnp.where(t == GROUPS - 1, ORDER[-1][1], (SIDES >> (2 * jnp.minimum(t, GROUPS - 2))) & 3)
        return jnp.where(half == 0, dz, jnp.where(dz == 4, 0, 8 - dz)), dy

    def target(t, half):
        dz, dy = turn_of(t, half)
        return 4 * ((my_z + dz) & 7) + ((my_y + dy) & 3)

    def arrived(t, half):
        dz, dy = turn_of(t, half)
        return 4 * ((my_z + 8 - dz) & 7) + ((my_y + 4 - dy) & 3)

    def each_other(act):
        def some(t, carry):
            for i in range(8):
                act((me + n // 2 + t * 8 + i) & (n - 1))
            return carry

        lax.fori_loop(0, n // 16, some, 0)
        for i in range(1, 8):
            act((me + i) & (n - 1))
        lax.fori_loop(n // 16 + 1, n // 8, some, 0)

    def near_first(act):
        def some(t, carry):
            at = (jnp.where(t < 7, NEARS[0], NEARS[1]) >> (4 * jnp.where(t < 7, t, t - 7))) & 15
            for i in range(8):
                act((me + at * 8 + i) & (n - 1))
            return carry

        lax.fori_loop(0, 14, some, 0)
        for i in range(1, 8):
            act((me + i) & (n - 1))
        for i in range(8):
            act((me + NEAR[14] * 8 + i) & (n - 1))

    barrier = pltpu.get_barrier_semaphore()
    each_other(lambda to: pl.semaphore_signal(barrier, 1, device_id={"dev": to}, device_id_type=MESH))
    copies = [pltpu.make_async_copy(tables_hbm, tables_ref, local_sems.at[4])] + [
        pltpu.make_async_copy(top_hbm.at[:, pl.ds(at * 128, 128)], raw_ref.at[at], local_sems.at[at])
        for at in range(4)
    ]
    for copy in copies:
        copy.start()

    prep_ids(rows_ref, lens_ref, counts_ref, ids_out)
    ids_in[me] = ids_out[me]
    pl.semaphore_wait(barrier, n - 1)

    def id_copy(src, dst, to, group):
        return pltpu.make_async_remote_copy(
            src_ref=src, dst_ref=dst, send_sem=send_sem.at[1], recv_sem=ids_sems.at[group],
            device_id={"dev": to}, device_id_type=MESH,
        )

    near_first(lambda to: id_copy(ids_out.at[to], ids_in.at[me], to, my_chunk).start())
    copies[0].wait()
    pool_turn(tables_ref, turned_ref)
    for copy in copies[1:]:
        copy.wait()

    def ids_of(group, count):
        some = pl.ds(0, count)
        return id_copy(ids_out.at[some], ids_in.at[some], (me + 1) % n, group)

    def row_copy(src, dst, to, chunk):
        return pltpu.make_async_remote_copy(
            src_ref=src, dst_ref=dst, send_sem=send_sem.at[0], recv_sem=recv_sems.at[chunk],
            device_id={"dev": to}, device_id_type=MESH,
        )

    def block(ref, device):
        return ref.at[pl.ds(pl.multiple_of(device * ROOM, ROOM), ROOM), :]

    def wait_ids(chunk):
        @pl.when(chunk == my_chunk)
        def _():
            ids_of(chunk, 3).wait_recv()

        @pl.when(chunk != my_chunk)
        def _():
            ids_of(chunk, 4).wait_recv()

    def step(t, carry):
        chunks = [target(t, half) for half in range(2)]
        for half in range(2):
            wait_ids(chunks[half])
            ids_wide[half * 4 : half * 4 + 4] = ids_in[
                pl.ds(pl.multiple_of(chunks[half] * 4, 4), 4)
            ].astype(I32)
        pool_setup(
            lambda q, j: ids_wide[pl.ds(q, 2, stride=4), j, :], y_ref, code_ref, pos_ref, scale_ref
        )
        for j in range(4):
            pool_table(j, turned_ref, y_ref, code_ref, scale_ref, xt_ref)
        blocks = pool_pack(pos_ref, xt_ref)
        for half in range(2):
            send_ref[pl.ds(pl.multiple_of(chunks[half] * 4 * ROOM, 4 * ROOM), 4 * ROOM), :] = blocks[half]
        for u in range(2):
            weight_cut(2 * t + u, raw_ref, plane_ref)

        for i in range(4):
            for half in range(2):
                to = chunks[half] * 4 + ((my_place + i) & 3)

                @pl.when(to != me)
                def _():
                    row_copy(block(send_ref, to), block(recv_ref, me), to, my_chunk).start()

        return carry

    lax.fori_loop(0, GROUPS, step, 0)
    target_setup(inverse_ref, counts_ref, order_ref, compress_ref, turn_ref, mix_ref)
    perm_ref[...] = order_columns(order_ref).astype(F32).T.astype(BF)
    for c in range(2 * GROUPS):
        cols_ref[c] = mix_ref[:, c * 16 : c * 16 + 16]

    def clear(w, carry):
        rows = pl.ds(pl.multiple_of(arrived(GROUPS - 4 + w // 2, w % 2) * 16, 16), 16)
        feat_ref[:, :, rows, :] = jnp.zeros((64, 2, 16, 128), BF)
        return carry

    lax.fori_loop(0, 8, clear, 0)
    mine = pl.ds(pl.multiple_of(me * ROOM, ROOM), ROOM)
    recv_ref[mine, :] = send_ref[mine, :]

    def take(u, v):
        chunk = arrived(u, v)

        @pl.when(chunk == my_chunk)
        def _():
            rows = pl.ds(0, 3 * ROOM)
            row_copy(send_ref.at[rows, :], recv_ref.at[rows, :], (me + 1) % n, chunk).wait_recv()

        @pl.when(chunk != my_chunk)
        def _():
            rows = pl.ds(0, 4 * ROOM)
            row_copy(send_ref.at[rows, :], recv_ref.at[rows, :], (me + 1) % n, chunk).wait_recv()

        pick_chunk(chunk, recv_ref, turn_ref, feat_ref)

    def turn_and_take(w, carry):
        weight_plane(w, perm_ref, plane_ref, raw_ref)
        take(w // 2, w % 2)
        return carry

    def only_take(w, carry):
        take(w // 2, w % 2)
        return carry

    lax.fori_loop(0, 16, turn_and_take, 0)
    lax.fori_loop(16, 2 * GROUPS - 8, only_take, 0)

    def keep(i, value):
        sum_ref[i] = value

    mixing(mix_ref[...], lambda i, v: feat_ref[i, v], keep)
    lax.fori_loop(2 * GROUPS - 8, 2 * GROUPS, only_take, 0)
    last = [arrived(GROUPS - 4 + w // 2, w % 2) for w in range(8)]
    zero = jnp.zeros((16, 128), BF)

    def settle(i, value):
        mixed = (sum_ref[i] + value).astype(BF)
        for v in range(2):
            left_ref[i, v, v * 16 : v * 16 + 16, :] = mixed[:, v * 128 : v * 128 + 128]
            left_ref[i, v, 16 - v * 16 : 32 - v * 16, :] = zero

    mixing(
        jnp.concatenate([cols_ref[c] for c in last], axis=1),
        lambda i, v: jnp.concatenate(
            [feat_ref[i, v, pl.ds(pl.multiple_of(c * 16, 16), 16), :] for c in last], axis=0
        ),
        settle,
    )
    finish(
        feat_ref, lambda k, at: raw_ref[at, pl.ds(pl.multiple_of(k * 512, 512), 512), :],
        bias_ref, out_ref, left_ref, pair_ref, acc_ref,
    )
    ids_of(my_chunk, n - 1).wait_send()
    rows = pl.ds(0, (n - 1) * ROOM)
    row_copy(send_ref.at[rows, :], recv_ref.at[rows, :], (me + 1) % n, my_chunk).wait_send()


def shards(tables, bag_rows, bag_lengths, row_counts, inverse, table_order, compress, top_weight, top_bias):
    order = table_order.reshape(1, -1)
    bias = top_bias.reshape(1, -1)
    rows = bag_rows[0].transpose(1, 2, 0)
    lens = bag_lengths[0].transpose(1, 0)
    samples, units = inverse.shape[0], top_weight.shape[1]
    anywhere = pl.BlockSpec(memory_space=pl.ANY)
    scratch = (
        [pltpu.VMEM(tables.shape, BF)]
        + pool_scratch()
        + [
            pltpu.VMEM((units // 128, top_weight.shape[0], 128), BF),
            pltpu.VMEM((16, units // 128, 512, 128), BF),
            pltpu.VMEM((512, 512), BF),
            pltpu.VMEM((128, 4, 128), jnp.int16),
            pltpu.VMEM((128, 4, 128), jnp.int16),
            pltpu.VMEM((8, 4, 128), I32),
            pltpu.VMEM((128 * ROOM, 128), BF),
            pltpu.VMEM((128 * ROOM, 128), BF),
        ]
        + score_scratch()
        + [pltpu.VMEM((2 * GROUPS, 16, 16), BF)]
        + [
            pltpu.SemaphoreType.DMA((5,)),
            pltpu.SemaphoreType.DMA((2 * GROUPS,)),
            pltpu.SemaphoreType.DMA((2,)),
            pltpu.SemaphoreType.DMA((2 * GROUPS,)),
        ]
    )
    hidden = pl.pallas_call(
        lookup_body,
        out_shape=jax.ShapeDtypeStruct((samples, units), F32),
        in_specs=[VM] * 7 + [anywhere] * 2,
        out_specs=VM,
        scratch_shapes=scratch,
        compiler_params=pltpu.CompilerParams(vmem_limit_bytes=BIG, collective_id=0, has_side_effects=True),
        cost_estimate=pl.CostEstimate(flops=3 * 10**10, bytes_accessed=16 << 20, transcendentals=0),
    )(rows, lens, row_counts, inverse, order, compress, bias, tables, top_weight)
    return jnp.maximum(hidden, 0.0).astype(BF)


def solution(mesh):
    return jax.shard_map(
        shards,
        mesh=mesh,
        in_specs=(
            P("dev", None, None),
            P(("rep", "dev"), None, None, None),
            P(("rep", "dev"), None, None),
            P(("rep", "dev"), None),
            P(("rep", "dev"), None),
            P(),
            P(),
            P(),
            P(),
        ),
        out_specs=P(("rep", "dev"), None),
        check_vma=False,
    )
```

```python
import functools
import jax
import jax.numpy as jnp
from jax import lax
from jax.experimental import pallas as pl
from jax.experimental.pallas import tpu as pltpu
from jax.sharding import PartitionSpec as P

BF = jnp.bfloat16
F32 = jnp.float32
I32 = jnp.int32
ROOM = 80


def iota(shape, axis):
    return lax.broadcasted_iota(I32, shape, axis)


def onehot(mask):
    return jnp.where(mask, 1.0, 0.0).astype(BF)


def prep_ids(rows_ref, lens_ref, counts_ref, ids_out):
    most, pool, slots = rows_ref.shape
    used = iota((most, slots), 0) < counts_ref[...]
    lens = lens_ref[...]
    wide = jnp.concatenate(
        [jnp.where(used & (p < lens), rows_ref[:, p, :], -1) for p in range(pool)], axis=0
    )
    for at in range(slots // 128):
        turned = wide[:, at * 128 : (at + 1) * 128].T.reshape(32, 4, 128)
        ids_out[at * 32 : at * 32 + 32] = turned.astype(jnp.int16)


PLANE = 128


def pool_turn(tables_ref, turned_ref):
    tabs, vocab, width = tables_ref.shape
    for j in range(tabs):
        for at in range(vocab // 128):
            turned_ref[j, at] = (
                tables_ref[j, at * 128 : at * 128 + 128, :].astype(F32).T * (0.25 ** (at % 4))
            ).astype(BF)


def pool_setup(load_ids, y_ref, code_ref, pos_ref, scale_ref):
    lane = iota((2, 128), 1)
    chunk = lane // 32
    same = onehot(iota((128, 128), 0) // 32 == iota((128, 128), 1) // 32)
    base = jnp.zeros((2, 128), F32)
    for j in range(4):
        got = [load_ids(q, j) for q in range(4)]
        ys = []
        for p in range(4):
            y = got[0] if p == 0 else pltpu.roll(got[0], (-p * 32) % 128, 1)
            for q in range(1, 4):
                moved = got[q] if p == q else pltpu.roll(got[q], ((q - p) * 32) % 128, 1)
                y = jnp.where(chunk == q, moved, y)
            ys.append(y)
        valid = ys[0] >= 0
        total = jnp.dot(onehot(valid), same, preferred_element_type=F32)
        place = base.astype(I32) + (lane % 32) + chunk * ROOM
        pos_ref[j * 8 : j * 8 + 2, :] = jnp.where(valid, place, -1)
        base = base + total
        alike = (ys[0] == ys[1]) & (ys[0] == ys[2]) & (ys[0] == ys[3])
        scale_ref[j * 8 : j * 8 + 2, :] = jnp.where(alike, 2.0, 1.0)
        for p in range(4):
            y = ys[p]
            live = (y >= 0) if p < 2 else ((y >= 0) & ~alike)
            code = jnp.where(live, jnp.left_shift(jnp.ones_like(y), ((y >> 7) * 2) & 31), 0)
            at = (j * 4 + p) * 8
            y_ref[at : at + 2, :] = y & 127
            for k in range(4):
                code_ref[k * PLANE + at : k * PLANE + at + 2, :] = (
                    lax.shift_right_logical(code, jnp.full_like(code, 8 * k)) & 255
                )


def small(ref, at):
    return jnp.broadcast_to(ref[pl.ds(at, 1), :], (16, 128)).astype(jnp.int16)


def pool_table(j, turned_ref, y_ref, code_ref, scale_ref, xt_ref):
    low_iota = iota((16, 128), 0).astype(jnp.int16)
    zero = jnp.zeros((16, 128), jnp.int16)
    rows = [[(j * 4 + p) * 8 + half for p in range(4)] for half in range(2)]
    hits = []
    for half in range(2):
        lows = [small(y_ref, row) for row in rows[half]]
        hits.append([[low == low_iota + jnp.int16(16 * at) for low in lows] for at in range(8)])
    total = None
    for k in range(4):
        planes = []
        for half in range(2):
            codes = [small(code_ref, k * PLANE + row) for row in rows[half]]
            plane = []
            for hit in hits[half]:
                cut = [jnp.where(hit[p], codes[p], zero) for p in range(4)]
                plane.append((cut[0] + cut[1]) + (cut[2] + cut[3]))
            planes.append(jnp.concatenate(plane, axis=0).astype(jnp.uint8))
        for i in (0, 2):
            hot = jnp.concatenate(
                [
                    jnp.concatenate([(plane & jnp.uint8(3 << (2 * u))).astype(BF) for u in (i, i + 1)], axis=0)
                    for plane in planes
                ],
                axis=1,
            )
            left = jnp.concatenate([turned_ref[j, 4 * k + i], turned_ref[j, 4 * k + i + 1]], axis=1)
            part = jnp.dot(left, hot, preferred_element_type=F32)
            total = part if total is None else total + part
    for half in range(2):
        scale = scale_ref[pl.ds(j * 8 + half, 1), :]
        xt_ref[half, j] = (total[:, half * 128 : half * 128 + 128] * scale).astype(BF)


def pool_pack(pos_ref, xt_ref):
    out = []
    for half in range(2):
        total = None
        for jj in range(2):
            packs, cols = [], []
            for j in (2 * jj, 2 * jj + 1):
                pos = small(pos_ref, j * 8 + half)
                hits = [
                    jnp.where(
                        pos == iota((16, 128), 0).astype(jnp.int16) + jnp.int16(16 * at),
                        jnp.ones((16, 128), BF),
                        jnp.zeros((16, 128), BF),
                    )
                    for at in range(4 * ROOM // 16)
                ]
                packs.append(jnp.concatenate(hits, axis=0))
                cols.append(xt_ref[half, j])
            part = lax.dot_general(
                jnp.concatenate(packs, axis=1),
                jnp.concatenate(cols, axis=1),
                (((1,), (1,)), ((), ())),
                preferred_element_type=F32,
            )
            total = part if total is None else total + part
        out.append(total.astype(BF))
    return out


def pool_scratch():
    return [
        pltpu.VMEM((4, 16, 128, 128), BF),
        pltpu.VMEM((PLANE, 128), I32),
        pltpu.VMEM((4 * PLANE, 128), I32),
        pltpu.VMEM((32, 128), I32),
        pltpu.VMEM((32, 128), F32),
        pltpu.VMEM((2, 4, 128, 128), BF),
    ]


def order_columns(order_ref):
    slots = order_ref.shape[1]
    return onehot(iota((slots, slots), 0) == order_ref[...])


def weight_cut(at, raw_ref, plane_ref):
    row = iota((256, 256), 0)
    col = iota((256, 256), 1)
    spread = onehot((col % 16 == row // 16) & (col // 16 == row % 16))
    rows = pl.ds(pl.multiple_of(at * 256, 256), 256)
    block = jnp.dot(
        spread, jnp.concatenate([raw_ref[c, rows, :] for c in range(4)], axis=1), preferred_element_type=F32
    ).astype(BF)
    for k in range(16):
        for c in range(4):
            plane_ref[k, c, pl.ds(pl.multiple_of(at * 16, 16), 16), :] = block[
                k * 16 : k * 16 + 16, c * 128 : c * 128 + 128
            ]


def weight_plane(k, perm_ref, plane_ref, raw_ref):
    plane = jnp.concatenate([plane_ref[k, c] for c in range(4)], axis=1)
    done = jnp.dot(perm_ref[...], plane, preferred_element_type=F32).astype(BF)
    for c in range(4):
        raw_ref[c, pl.ds(pl.multiple_of(k * 512, 512), 512), :] = done[:, c * 128 : c * 128 + 128]


def target_setup(inverse_ref, counts_ref, order_ref, compress_ref, turn_ref, mix_ref):
    samples, slots = inverse_ref.shape
    columns = order_columns(order_ref)
    mix_ref[...] = jnp.dot(compress_ref[...], columns, preferred_element_type=F32).astype(BF)
    chosen = jnp.dot(inverse_ref[...].astype(F32).astype(BF), columns, preferred_element_type=F32)
    counts = jnp.broadcast_to(counts_ref[...], (16, slots)).astype(F32)
    before = (iota((slots, slots), 0) // 4 == iota((slots, slots), 1) // 4) & (
        iota((slots, slots), 0) < iota((slots, slots), 1)
    )
    base = jnp.dot(counts.astype(BF), onehot(before), preferred_element_type=F32)[:1, :]
    offset = ((iota((1, slots), 1) // 4) % 2 * ROOM).astype(F32)
    place = jnp.where(chosen < counts[:1, :], chosen + (base + offset), 255.0)
    for at in range(slots // 128):
        turned = place[:, at * 128 : (at + 1) * 128].T.astype(I32).reshape(8, 16, 128)
        upper, lower = turned[:, :8].reshape(64, 128), turned[:, 8:].reshape(64, 128)
        two = upper | (lower << 8)
        turn_ref[pl.ds(at * 64, 64), :] = two | (pltpu.roll(two, 64, 1) << 16)


def pick_chunk(c, packed_ref, turn_ref, feat_ref):
    place = turn_ref[pl.ds(pl.multiple_of(c * 8, 8), 8), :]
    near = iota((16, 128), 1).astype(jnp.int16)
    far = near + jnp.int16(128)
    one, zero = jnp.ones((16, 128), BF), jnp.zeros((16, 128), BF)
    rows = jnp.concatenate(
        [packed_ref[pl.ds(pl.multiple_of(c * 320 + h * 160, 160), 160), :] for h in range(2)], axis=1
    )
    at = pl.ds(pl.multiple_of(c * 16, 16), 16)
    for part in range(4):
        left, right = [[], []], [[], []]
        for b in range(part * 16, part * 16 + 16):
            x = jnp.broadcast_to(place[:, b : b + 1], (8, 128))
            for v in range(2):
                cut = [(x >> (16 * v)) & 255, (x >> (16 * v + 8)) & 255]
                want = jnp.concatenate(cut, axis=0).astype(jnp.int16)
                left[v].append(jnp.where(want == near, one, zero))
                right[v].append(jnp.where(want == far, one, zero)[:, :32])
        got = jnp.dot(
            jnp.concatenate(
                [jnp.concatenate(left[0] + left[1], axis=0), jnp.concatenate(right[0] + right[1], axis=0)], axis=1
            ),
            rows,
            preferred_element_type=F32,
        ).reshape(2, 16, 16, 256)
        both = jnp.concatenate([got[:, :, :8, :128], got[:, :, 8:, 128:]], axis=2).astype(BF)
        for v in range(2):
            feat_ref[part * 16 : part * 16 + 16, v, at, :] = both[v]


def mixing(columns, feats_of, store):
    def some(i, carry):
        for u in range(16):
            feats = jnp.concatenate([feats_of(i * 16 + u, v) for v in range(2)], axis=1)
            store(i * 16 + u, jnp.dot(columns, feats, preferred_element_type=F32))
        return carry

    lax.fori_loop(0, 4, some, 0)


def finish(feat_ref, weight_at, bias_ref, out_ref, left_ref, pair_ref, acc_ref):
    def pairing(i, carry):
        for u in range(32):
            sides = [
                jnp.concatenate([ref[i * 32 + u, v] for v in range(2)], axis=1) for ref in (left_ref, feat_ref)
            ]
            both = lax.dot_general(
                sides[0], sides[1], (((1,), (1,)), ((), ())), preferred_element_type=F32
            )
            for v in range(2):
                to = pl.ds(pl.multiple_of((v * 64 + i * 32 + u) * 24, 8), 16)
                for at in range(4):
                    pair_ref[at, to, :] = both[v * 16 : v * 16 + 16, at * 128 : at * 128 + 128]
        return carry

    lax.fori_loop(0, 2, pairing, 0)
    acc_ref[...] = jnp.broadcast_to(bias_ref[...], acc_ref.shape)

    def plane(i, carry):
        total = acc_ref[...]
        for u in range(8):
            k = i * 8 + u
            lhs = jnp.concatenate(
                [pair_ref[at, pl.ds(k, 128, stride=24), :].astype(BF) for at in range(4)], axis=1
            )
            total = total + jnp.dot(
                lhs, jnp.concatenate([weight_at(k, at) for at in range(4)], axis=1), preferred_element_type=F32)
        acc_ref[...] = total
        return carry

    lax.fori_loop(0, 2, plane, 0)
    out_ref[...] = acc_ref[...]


def score_scratch():
    return [
        pltpu.VMEM((256, 128), I32),
        pltpu.VMEM((16, 512), BF),
        pltpu.VMEM((64, 2, 512, 128), BF),
        pltpu.VMEM((64, 2, 32, 128), BF),
        pltpu.VMEM((64, 16, 256), F32),
        pltpu.VMEM((4, 3072, 128), F32),
        pltpu.VMEM((128, 512), F32),
    ]


VM = pl.BlockSpec(memory_space=pltpu.VMEM)
BIG = 56 * 1024 * 1024


MESH = pl.DeviceIdType.MESH
GROUPS = 16
ORDER = [(1, 0), (1, 1)] + [(4, y) for y in range(4)] + [(3, y) for y in range(4)] + [(2, y) for y in range(4)]
ORDER += [(1, 2), (1, 3)]
SHIFTS = [sum(ORDER[8 * part + at][0] << (3 * at) for at in range(8)) for part in range(2)]
SIDES = sum(dy << (2 * at) for at, (_, dy) in enumerate(ORDER[:15]))
NEAR = [13, 14, 1, 2, 12, 15, 3, 4, 11, 5, 10, 6, 9, 7, 8]
NEARS = [sum(part[at] << (4 * at) for at in range(len(part))) for part in (NEAR[:7], NEAR[7:14])]


def lookup_body(
    rows_hbm, lens_hbm, counts_hbm, inverse_hbm, order_hbm, compress_hbm, bias_hbm, tables_hbm, top_hbm,
    out_ref,
    rows_ref, lens_ref, counts_ref, inverse_ref, order_ref, compress_ref, bias_ref,
    tables_ref, turned_ref, y_ref, code_ref, pos_ref, scale_ref, xt_ref,
    raw_ref, plane_ref, perm_ref, ids_out, ids_in, ids_wide, send_ref, recv_ref,
    turn_ref, mix_ref, feat_ref, left_ref, sum_ref, pair_ref, acc_ref, cols_ref,
    local_sems, ids_sems, send_sem, recv_sems,
):
    n = 8 * GROUPS
    me = lax.axis_index("dev")
    my_place, my_chunk = me & 3, me // 4
    my_z, my_y = my_chunk // 4, my_chunk & 3

    def turn_of(t, half):
        dz = (jnp.where(t < 8, SHIFTS[0], SHIFTS[1]) >> (3 * (t & 7))) & 7
        dy = jnp.where(t == GROUPS - 1, ORDER[-1][1], (SIDES >> (2 * jnp.minimum(t, GROUPS - 2))) & 3)
        return jnp.where(half == 0, dz, jnp.where(dz == 4, 0, 8 - dz)), dy

    def target(t, half):
        dz, dy = turn_of(t, half)
        return 4 * ((my_z + dz) & 7) + ((my_y + dy) & 3)

    def arrived(t, half):
        dz, dy = turn_of(t, half)
        return 4 * ((my_z + 8 - dz) & 7) + ((my_y + 4 - dy) & 3)

    def each_other(act):
        def some(t, carry):
            for i in range(8):
                act((me + n // 2 + t * 8 + i) & (n - 1))
            return carry

        lax.fori_loop(0, n // 16, some, 0)
        for i in range(1, 8):
            act((me + i) & (n - 1))
        lax.fori_loop(n // 16 + 1, n // 8, some, 0)

    def near_first(act):
        def some(t, carry):
            at = (jnp.where(t < 7, NEARS[0], NEARS[1]) >> (4 * jnp.where(t < 7, t, t - 7))) & 15
            for i in range(8):
                act((me + at * 8 + i) & (n - 1))
            return carry

        lax.fori_loop(0, 14, some, 0)
        for i in range(1, 8):
            act((me + i) & (n - 1))
        for i in range(8):
            act((me + NEAR[14] * 8 + i) & (n - 1))

    small_copies = [
        pltpu.make_async_copy(src, dst, local_sems.at[5 + at])
        for at, (src, dst) in enumerate(
            (
                (rows_hbm, rows_ref), (lens_hbm, lens_ref), (counts_hbm, counts_ref), (inverse_hbm, inverse_ref),
                (order_hbm, order_ref), (compress_hbm, compress_ref), (bias_hbm, bias_ref),
            )
        )
    ]
    for copy in small_copies:
        copy.start()
    barrier = pltpu.get_barrier_semaphore()
    each_other(lambda to: pl.semaphore_signal(barrier, 1, device_id={"dev": to}, device_id_type=MESH))
    copies = [pltpu.make_async_copy(tables_hbm, tables_ref, local_sems.at[4])] + [
        pltpu.make_async_copy(top_hbm.at[:, pl.ds(at * 128, 128)], raw_ref.at[at], local_sems.at[at])
        for at in range(4)
    ]
    for copy in copies:
        copy.start()

    for copy in small_copies[:3]:
        copy.wait()
    prep_ids(rows_ref, lens_ref, counts_ref, ids_out)
    ids_in[me] = ids_out[me]
    pl.semaphore_wait(barrier, n - 1)

    def id_copy(src, dst, to, group):
        return pltpu.make_async_remote_copy(
            src_ref=src, dst_ref=dst, send_sem=send_sem.at[1], recv_sem=ids_sems.at[group],
            device_id={"dev": to}, device_id_type=MESH,
        )

    near_first(lambda to: id_copy(ids_out.at[to], ids_in.at[me], to, my_chunk).start())
    copies[0].wait()
    pool_turn(tables_ref, turned_ref)
    for copy in copies[1:] + small_copies[3:]:
        copy.wait()

    def ids_of(group, count):
        some = pl.ds(0, count)
        return id_copy(ids_out.at[some], ids_in.at[some], (me + 1) % n, group)

    def row_copy(src, dst, to, chunk):
        return pltpu.make_async_remote_copy(
            src_ref=src, dst_ref=dst, send_sem=send_sem.at[0], recv_sem=recv_sems.at[chunk],
            device_id={"dev": to}, device_id_type=MESH,
        )

    def block(ref, device):
        return ref.at[pl.ds(pl.multiple_of(device * ROOM, ROOM), ROOM), :]

    def wait_ids(chunk):
        @pl.when(chunk == my_chunk)
        def _():
            ids_of(chunk, 3).wait_recv()

        @pl.when(chunk != my_chunk)
        def _():
            ids_of(chunk, 4).wait_recv()

    def step(t, carry):
        chunks = [target(t, half) for half in range(2)]
        for half in range(2):
            wait_ids(chunks[half])
            ids_wide[half * 4 : half * 4 + 4] = ids_in[
                pl.ds(pl.multiple_of(chunks[half] * 4, 4), 4)
            ].astype(I32)
        pool_setup(
            lambda q, j: ids_wide[pl.ds(q, 2, stride=4), j, :], y_ref, code_ref, pos_ref, scale_ref
        )
        for j in range(4):
            pool_table(j, turned_ref, y_ref, code_ref, scale_ref, xt_ref)
        blocks = pool_pack(pos_ref, xt_ref)
        for half in range(2):
            send_ref[pl.ds(pl.multiple_of(chunks[half] * 4 * ROOM, 4 * ROOM), 4 * ROOM), :] = blocks[half]
        for u in range(2):
            weight_cut(2 * t + u, raw_ref, plane_ref)

        for i in range(4):
            for half in range(2):
                to = chunks[half] * 4 + ((my_place + i) & 3)

                @pl.when(to != me)
                def _():
                    row_copy(block(send_ref, to), block(recv_ref, me), to, my_chunk).start()

        return carry

    lax.fori_loop(0, GROUPS, step, 0)
    target_setup(inverse_ref, counts_ref, order_ref, compress_ref, turn_ref, mix_ref)
    perm_ref[...] = order_columns(order_ref).astype(F32).T.astype(BF)
    for c in range(2 * GROUPS):
        cols_ref[c] = mix_ref[:, c * 16 : c * 16 + 16]

    def clear(w, carry):
        rows = pl.ds(pl.multiple_of(arrived(GROUPS - 4 + w // 2, w % 2) * 16, 16), 16)
        feat_ref[:, :, rows, :] = jnp.zeros((64, 2, 16, 128), BF)
        return carry

    lax.fori_loop(0, 8, clear, 0)
    mine = pl.ds(pl.multiple_of(me * ROOM, ROOM), ROOM)
    recv_ref[mine, :] = send_ref[mine, :]

    def take(u, v):
        chunk = arrived(u, v)

        @pl.when(chunk == my_chunk)
        def _():
            rows = pl.ds(0, 3 * ROOM)
            row_copy(send_ref.at[rows, :], recv_ref.at[rows, :], (me + 1) % n, chunk).wait_recv()

        @pl.when(chunk != my_chunk)
        def _():
            rows = pl.ds(0, 4 * ROOM)
            row_copy(send_ref.at[rows, :], recv_ref.at[rows, :], (me + 1) % n, chunk).wait_recv()

        pick_chunk(chunk, recv_ref, turn_ref, feat_ref)

    def turn_and_take(w, carry):
        weight_plane(w, perm_ref, plane_ref, raw_ref)
        take(w // 2, w % 2)
        return carry

    def only_take(w, carry):
        take(w // 2, w % 2)
        return carry

    lax.fori_loop(0, 16, turn_and_take, 0)
    lax.fori_loop(16, 2 * GROUPS - 8, only_take, 0)

    def keep(i, value):
        sum_ref[i] = value

    mixing(mix_ref[...], lambda i, v: feat_ref[i, v], keep)
    lax.fori_loop(2 * GROUPS - 8, 2 * GROUPS, only_take, 0)
    last = [arrived(GROUPS - 4 + w // 2, w % 2) for w in range(8)]
    zero = jnp.zeros((16, 128), BF)

    def settle(i, value):
        mixed = (sum_ref[i] + value).astype(BF)
        for v in range(2):
            left_ref[i, v, v * 16 : v * 16 + 16, :] = mixed[:, v * 128 : v * 128 + 128]
            left_ref[i, v, 16 - v * 16 : 32 - v * 16, :] = zero

    mixing(
        jnp.concatenate([cols_ref[c] for c in last], axis=1),
        lambda i, v: jnp.concatenate(
            [feat_ref[i, v, pl.ds(pl.multiple_of(c * 16, 16), 16), :] for c in last], axis=0
        ),
        settle,
    )
    finish(
        feat_ref, lambda k, at: raw_ref[at, pl.ds(pl.multiple_of(k * 512, 512), 512), :],
        bias_ref, out_ref, left_ref, pair_ref, acc_ref,
    )
    ids_of(my_chunk, n - 1).wait_send()
    rows = pl.ds(0, (n - 1) * ROOM)
    row_copy(send_ref.at[rows, :], recv_ref.at[rows, :], (me + 1) % n, my_chunk).wait_send()


def shards(tables, bag_rows, bag_lengths, row_counts, inverse, table_order, compress, top_weight, top_bias):
    order = table_order.reshape(1, -1)
    bias = top_bias.reshape(1, -1)
    rows = bag_rows[0].transpose(1, 2, 0)
    lens = bag_lengths[0].transpose(1, 0)
    samples, units = inverse.shape[0], top_weight.shape[1]
    anywhere = pl.BlockSpec(memory_space=pl.ANY)
    scratch = (
        [pltpu.VMEM(x.shape, x.dtype) for x in (rows, lens, row_counts, inverse, order, compress, bias)]
        + [pltpu.VMEM(tables.shape, BF)]
        + pool_scratch()
        + [
            pltpu.VMEM((units // 128, top_weight.shape[0], 128), BF),
            pltpu.VMEM((16, units // 128, 512, 128), BF),
            pltpu.VMEM((512, 512), BF),
            pltpu.VMEM((128, 4, 128), jnp.int16),
            pltpu.VMEM((128, 4, 128), jnp.int16),
            pltpu.VMEM((8, 4, 128), I32),
            pltpu.VMEM((128 * ROOM, 128), BF),
            pltpu.VMEM((128 * ROOM, 128), BF),
        ]
        + score_scratch()
        + [pltpu.VMEM((2 * GROUPS, 16, 16), BF)]
        + [
            pltpu.SemaphoreType.DMA((12,)),
            pltpu.SemaphoreType.DMA((2 * GROUPS,)),
            pltpu.SemaphoreType.DMA((2,)),
            pltpu.SemaphoreType.DMA((2 * GROUPS,)),
        ]
    )
    hidden = pl.pallas_call(
        lookup_body,
        out_shape=jax.ShapeDtypeStruct((samples, units), F32),
        in_specs=[anywhere] * 9,
        out_specs=VM,
        scratch_shapes=scratch,
        compiler_params=pltpu.CompilerParams(vmem_limit_bytes=BIG, collective_id=0, has_side_effects=True),
        cost_estimate=pl.CostEstimate(flops=3 * 10**10, bytes_accessed=16 << 20, transcendentals=0),
    )(rows, lens, row_counts, inverse, order, compress, bias, tables, top_weight)
    return jnp.maximum(hidden, 0.0).astype(BF)


def solution(mesh):
    return jax.shard_map(
        shards,
        mesh=mesh,
        in_specs=(
            P("dev", None, None),
            P(("rep", "dev"), None, None, None),
            P(("rep", "dev"), None, None),
            P(("rep", "dev"), None),
            P(("rep", "dev"), None),
            P(),
            P(),
            P(),
            P(),
        ),
        out_specs=P(("rep", "dev"), None),
        check_vma=False,
    )
```

```python
import functools
import jax
import jax.numpy as jnp
from jax import lax
from jax.experimental import pallas as pl
from jax.experimental.pallas import tpu as pltpu
from jax.sharding import PartitionSpec as P

BF = jnp.bfloat16
F32 = jnp.float32
I32 = jnp.int32
ROOM = 80


def iota(shape, axis):
    return lax.broadcasted_iota(I32, shape, axis)


def onehot(mask):
    return jnp.where(mask, 1.0, 0.0).astype(BF)


def prep_ids(rows_ref, lens_ref, counts_ref, ids_out):
    most, pool, slots = rows_ref.shape
    used = iota((most, slots), 0) < counts_ref[...]
    lens = lens_ref[...]
    wide = jnp.concatenate(
        [jnp.where(used & (p < lens), rows_ref[:, p, :], -1) for p in range(pool)], axis=0
    )
    for at in range(slots // 128):
        turned = wide[:, at * 128 : (at + 1) * 128].T.reshape(32, 4, 128)
        ids_out[at * 32 : at * 32 + 32] = turned.astype(jnp.int16)


PLANE = 128


def pool_turn(tables_ref, turned_ref):
    tabs, vocab, width = tables_ref.shape
    for j in range(tabs):
        for at in range(vocab // 128):
            turned_ref[j, at] = (
                tables_ref[j, at * 128 : at * 128 + 128, :].astype(F32).T * (0.25 ** (at % 4))
            ).astype(BF)


def pool_setup(load_ids, y_ref, code_ref, pos_ref, scale_ref):
    lane = iota((2, 128), 1)
    chunk = lane // 32
    same = onehot(iota((128, 128), 0) // 32 == iota((128, 128), 1) // 32)
    base = jnp.zeros((2, 128), F32)
    for j in range(4):
        got = [load_ids(q, j) for q in range(4)]
        ys = []
        for p in range(4):
            y = got[0] if p == 0 else pltpu.roll(got[0], (-p * 32) % 128, 1)
            for q in range(1, 4):
                moved = got[q] if p == q else pltpu.roll(got[q], ((q - p) * 32) % 128, 1)
                y = jnp.where(chunk == q, moved, y)
            ys.append(y)
        valid = ys[0] >= 0
        total = jnp.dot(onehot(valid), same, preferred_element_type=F32)
        place = base.astype(I32) + (lane % 32) + chunk * ROOM
        pos_ref[j * 8 : j * 8 + 2, :] = jnp.where(valid, place, -1)
        base = base + total
        alike = (ys[0] == ys[1]) & (ys[0] == ys[2]) & (ys[0] == ys[3])
        scale_ref[j * 8 : j * 8 + 2, :] = jnp.where(alike, 2.0, 1.0)
        for p in range(4):
            y = ys[p]
            live = (y >= 0) if p < 2 else ((y >= 0) & ~alike)
            code = jnp.where(live, jnp.left_shift(jnp.ones_like(y), ((y >> 7) * 2) & 31), 0)
            at = (j * 4 + p) * 8
            y_ref[at : at + 2, :] = y & 127
            for k in range(4):
                code_ref[k * PLANE + at : k * PLANE + at + 2, :] = (
                    lax.shift_right_logical(code, jnp.full_like(code, 8 * k)) & 255
                )


def small(ref, at):
    return jnp.broadcast_to(ref[pl.ds(at, 1), :], (16, 128)).astype(jnp.int16)


def pool_table(j, turned_ref, y_ref, code_ref, scale_ref, xt_ref):
    low_iota = iota((16, 128), 0).astype(jnp.int16)
    zero = jnp.zeros((16, 128), jnp.int16)
    rows = [[(j * 4 + p) * 8 + half for p in range(4)] for half in range(2)]
    hits = []
    for half in range(2):
        lows = [small(y_ref, row) for row in rows[half]]
        hits.append([[low == low_iota + jnp.int16(16 * at) for low in lows] for at in range(8)])
    total = None
    for k in range(4):
        planes = []
        for half in range(2):
            codes = [small(code_ref, k * PLANE + row) for row in rows[half]]
            plane = []
            for hit in hits[half]:
                cut = [jnp.where(hit[p], codes[p], zero) for p in range(4)]
                plane.append((cut[0] + cut[1]) + (cut[2] + cut[3]))
            planes.append(jnp.concatenate(plane, axis=0).astype(jnp.uint8))
        for i in (0, 2):
            hot = jnp.concatenate(
                [
                    jnp.concatenate([(plane & jnp.uint8(3 << (2 * u))).astype(BF) for u in (i, i + 1)], axis=0)
                    for plane in planes
                ],
                axis=1,
            )
            left = jnp.concatenate([turned_ref[j, 4 * k + i], turned_ref[j, 4 * k + i + 1]], axis=1)
            part = jnp.dot(left, hot, preferred_element_type=F32)
            total = part if total is None else total + part
    for half in range(2):
        scale = scale_ref[pl.ds(j * 8 + half, 1), :]
        xt_ref[half, j] = (total[:, half * 128 : half * 128 + 128] * scale).astype(BF)


def pool_pack(pos_ref, xt_ref):
    out = []
    for half in range(2):
        total = None
        for jj in range(2):
            packs, cols = [], []
            for j in (2 * jj, 2 * jj + 1):
                pos = small(pos_ref, j * 8 + half)
                hits = [
                    jnp.where(
                        pos == iota((16, 128), 0).astype(jnp.int16) + jnp.int16(16 * at),
                        jnp.ones((16, 128), BF),
                        jnp.zeros((16, 128), BF),
                    )
                    for at in range(4 * ROOM // 16)
                ]
                packs.append(jnp.concatenate(hits, axis=0))
                cols.append(xt_ref[half, j])
            part = lax.dot_general(
                jnp.concatenate(packs, axis=1),
                jnp.concatenate(cols, axis=1),
                (((1,), (1,)), ((), ())),
                preferred_element_type=F32,
            )
            total = part if total is None else total + part
        out.append(total.astype(BF))
    return out


def pool_scratch():
    return [
        pltpu.VMEM((4, 16, 128, 128), BF),
        pltpu.VMEM((PLANE, 128), I32),
        pltpu.VMEM((4 * PLANE, 128), I32),
        pltpu.VMEM((32, 128), I32),
        pltpu.VMEM((32, 128), F32),
        pltpu.VMEM((2, 4, 128, 128), BF),
    ]


def order_columns(order_ref):
    slots = order_ref.shape[1]
    return onehot(iota((slots, slots), 0) == order_ref[...])


def weight_cut(at, raw_ref, plane_ref):
    row = iota((256, 256), 0)
    col = iota((256, 256), 1)
    spread = onehot((col % 16 == row // 16) & (col // 16 == row % 16))
    rows = pl.ds(pl.multiple_of(at * 256, 256), 256)
    block = jnp.dot(
        spread, jnp.concatenate([raw_ref[c, rows, :] for c in range(4)], axis=1), preferred_element_type=F32
    ).astype(BF)
    for k in range(16):
        for c in range(4):
            plane_ref[k, c, pl.ds(pl.multiple_of(at * 16, 16), 16), :] = block[
                k * 16 : k * 16 + 16, c * 128 : c * 128 + 128
            ]


def weight_plane(k, perm_ref, plane_ref, raw_ref):
    plane = jnp.concatenate([plane_ref[k, c] for c in range(4)], axis=1)
    done = jnp.dot(perm_ref[...], plane, preferred_element_type=F32).astype(BF)
    for c in range(4):
        raw_ref[c, pl.ds(pl.multiple_of(k * 512, 512), 512), :] = done[:, c * 128 : c * 128 + 128]


def target_setup(inverse_ref, counts_ref, order_ref, compress_ref, turn_ref, mix_ref):
    samples, slots = inverse_ref.shape
    columns = order_columns(order_ref)
    mix_ref[...] = jnp.dot(compress_ref[...], columns, preferred_element_type=F32).astype(BF)
    chosen = jnp.dot(inverse_ref[...].astype(F32).astype(BF), columns, preferred_element_type=F32)
    counts = jnp.broadcast_to(counts_ref[...], (16, slots)).astype(F32)
    before = (iota((slots, slots), 0) // 4 == iota((slots, slots), 1) // 4) & (
        iota((slots, slots), 0) < iota((slots, slots), 1)
    )
    base = jnp.dot(counts.astype(BF), onehot(before), preferred_element_type=F32)[:1, :]
    offset = ((iota((1, slots), 1) // 4) % 2 * ROOM).astype(F32)
    place = jnp.where(chosen < counts[:1, :], chosen + (base + offset), 255.0)
    for at in range(slots // 128):
        turned = place[:, at * 128 : (at + 1) * 128].T.astype(I32).reshape(8, 16, 128)
        upper, lower = turned[:, :8].reshape(64, 128), turned[:, 8:].reshape(64, 128)
        two = upper | (lower << 8)
        turn_ref[pl.ds(at * 64, 64), :] = two | (pltpu.roll(two, 64, 1) << 16)


def pick_chunk(c, packed_ref, turn_ref, feat_ref):
    place = turn_ref[pl.ds(pl.multiple_of(c * 8, 8), 8), :]
    near = iota((16, 128), 1).astype(jnp.int16)
    far = near + jnp.int16(128)
    one, zero = jnp.ones((16, 128), BF), jnp.zeros((16, 128), BF)
    rows = jnp.concatenate(
        [packed_ref[pl.ds(pl.multiple_of(c * 320 + h * 160, 160), 160), :] for h in range(2)], axis=1
    )
    at = pl.ds(pl.multiple_of(c * 16, 16), 16)
    for part in range(4):
        left, right = [[], []], [[], []]
        for b in range(part * 16, part * 16 + 16):
            x = jnp.broadcast_to(place[:, b : b + 1], (8, 128))
            for v in range(2):
                cut = [(x >> (16 * v)) & 255, (x >> (16 * v + 8)) & 255]
                want = jnp.concatenate(cut, axis=0).astype(jnp.int16)
                left[v].append(jnp.where(want == near, one, zero))
                right[v].append(jnp.where(want == far, one, zero)[:, :32])
        got = jnp.dot(
            jnp.concatenate(
                [jnp.concatenate(left[0] + left[1], axis=0), jnp.concatenate(right[0] + right[1], axis=0)], axis=1
            ),
            rows,
            preferred_element_type=F32,
        ).reshape(2, 16, 16, 256)
        both = jnp.concatenate([got[:, :, :8, :128], got[:, :, 8:, 128:]], axis=2).astype(BF)
        for v in range(2):
            feat_ref[part * 16 : part * 16 + 16, v, at, :] = both[v]


def mixing(columns, feats_of, store):
    def some(i, carry):
        for u in range(16):
            feats = jnp.concatenate([feats_of(i * 16 + u, v) for v in range(2)], axis=1)
            store(i * 16 + u, jnp.dot(columns, feats, preferred_element_type=F32))
        return carry

    lax.fori_loop(0, 4, some, 0)


def finish(feat_ref, weight_at, bias_ref, out_ref, left_ref, pair_ref, acc_ref):
    def pairing(i, carry):
        for u in range(32):
            sides = [
                jnp.concatenate([ref[i * 32 + u, v] for v in range(2)], axis=1) for ref in (left_ref, feat_ref)
            ]
            both = lax.dot_general(
                sides[0], sides[1], (((1,), (1,)), ((), ())), preferred_element_type=F32
            )
            for v in range(2):
                to = pl.ds(pl.multiple_of((v * 64 + i * 32 + u) * 24, 8), 16)
                for at in range(4):
                    pair_ref[at, to, :] = both[v * 16 : v * 16 + 16, at * 128 : at * 128 + 128]
        return carry

    lax.fori_loop(0, 2, pairing, 0)
    acc_ref[...] = jnp.broadcast_to(bias_ref[...], acc_ref.shape)

    def plane(i, carry):
        total = acc_ref[...]
        for u in range(8):
            k = i * 8 + u
            lhs = jnp.concatenate(
                [pair_ref[at, pl.ds(k, 128, stride=24), :].astype(BF) for at in range(4)], axis=1
            )
            total = total + jnp.dot(
                lhs, jnp.concatenate([weight_at(k, at) for at in range(4)], axis=1), preferred_element_type=F32)
        acc_ref[...] = total
        return carry

    lax.fori_loop(0, 2, plane, 0)
    out_ref[...] = acc_ref[...]


def score_scratch():
    return [
        pltpu.VMEM((256, 128), I32),
        pltpu.VMEM((16, 512), BF),
        pltpu.VMEM((64, 2, 512, 128), BF),
        pltpu.VMEM((64, 2, 32, 128), BF),
        pltpu.VMEM((64, 16, 256), F32),
        pltpu.VMEM((4, 3200, 128), F32),
        pltpu.VMEM((128, 512), F32),
    ]


VM = pl.BlockSpec(memory_space=pltpu.VMEM)
BIG = 56 * 1024 * 1024


MESH = pl.DeviceIdType.MESH
GROUPS = 16
ORDER = [(1, 0), (1, 1)] + [(4, y) for y in range(4)] + [(3, y) for y in range(4)] + [(2, y) for y in range(4)]
ORDER += [(1, 2), (1, 3)]
SHIFTS = [sum(ORDER[8 * part + at][0] << (3 * at) for at in range(8)) for part in range(2)]
SIDES = sum(dy << (2 * at) for at, (_, dy) in enumerate(ORDER[:15]))
NEAR = [13, 14, 1, 2, 12, 15, 3, 4, 11, 5, 10, 6, 9, 7, 8]
NEARS = [sum(part[at] << (4 * at) for at in range(len(part))) for part in (NEAR[:7], NEAR[7:14])]


def lookup_body(
    rows_hbm, lens_hbm, counts_hbm, inverse_hbm, order_hbm, compress_hbm, bias_hbm, tables_hbm, top_hbm,
    out_ref,
    rows_ref, lens_ref, counts_ref, inverse_ref, order_ref, compress_ref, bias_ref,
    tables_ref, turned_ref, y_ref, code_ref, pos_ref, scale_ref, xt_ref,
    raw_ref, plane_ref, perm_ref, ids_out, ids_in, ids_wide, send_ref, recv_ref,
    turn_ref, mix_ref, feat_ref, left_ref, sum_ref, pair_ref, acc_ref, cols_ref,
    local_sems, ids_sems, send_sem, recv_sems,
):
    n = 8 * GROUPS
    me = lax.axis_index("dev")
    my_place, my_chunk = me & 3, me // 4
    my_z, my_y = my_chunk // 4, my_chunk & 3

    def turn_of(t, half):
        dz = (jnp.where(t < 8, SHIFTS[0], SHIFTS[1]) >> (3 * (t & 7))) & 7
        dy = jnp.where(t == GROUPS - 1, ORDER[-1][1], (SIDES >> (2 * jnp.minimum(t, GROUPS - 2))) & 3)
        return jnp.where(half == 0, dz, jnp.where(dz == 4, 0, 8 - dz)), dy

    def target(t, half):
        dz, dy = turn_of(t, half)
        return 4 * ((my_z + dz) & 7) + ((my_y + dy) & 3)

    def arrived(t, half):
        dz, dy = turn_of(t, half)
        return 4 * ((my_z + 8 - dz) & 7) + ((my_y + 4 - dy) & 3)

    def each_other(act):
        def some(t, carry):
            for i in range(8):
                act((me + n // 2 + t * 8 + i) & (n - 1))
            return carry

        lax.fori_loop(0, n // 16, some, 0)
        for i in range(1, 8):
            act((me + i) & (n - 1))
        lax.fori_loop(n // 16 + 1, n // 8, some, 0)

    def near_first(act):
        def some(t, carry):
            at = (jnp.where(t < 7, NEARS[0], NEARS[1]) >> (4 * jnp.where(t < 7, t, t - 7))) & 15
            for i in range(8):
                act((me + at * 8 + i) & (n - 1))
            return carry

        lax.fori_loop(0, 14, some, 0)
        for i in range(1, 8):
            act((me + i) & (n - 1))
        for i in range(8):
            act((me + NEAR[14] * 8 + i) & (n - 1))

    small_copies = [
        pltpu.make_async_copy(src, dst, local_sems.at[5 + at])
        for at, (src, dst) in enumerate(
            (
                (rows_hbm, rows_ref), (lens_hbm, lens_ref), (counts_hbm, counts_ref), (inverse_hbm, inverse_ref),
                (order_hbm, order_ref), (compress_hbm, compress_ref), (bias_hbm, bias_ref),
            )
        )
    ]
    for copy in small_copies:
        copy.start()
    barrier = pltpu.get_barrier_semaphore()
    each_other(lambda to: pl.semaphore_signal(barrier, 1, device_id={"dev": to}, device_id_type=MESH))
    copies = [pltpu.make_async_copy(tables_hbm, tables_ref, local_sems.at[4])] + [
        pltpu.make_async_copy(top_hbm.at[:, pl.ds(at * 128, 128)], raw_ref.at[at], local_sems.at[at])
        for at in range(4)
    ]
    for copy in copies:
        copy.start()

    for copy in small_copies[:3]:
        copy.wait()
    prep_ids(rows_ref, lens_ref, counts_ref, ids_out)
    ids_in[me] = ids_out[me]
    pl.semaphore_wait(barrier, n - 1)

    def id_copy(src, dst, to, group):
        return pltpu.make_async_remote_copy(
            src_ref=src, dst_ref=dst, send_sem=send_sem.at[1], recv_sem=ids_sems.at[group],
            device_id={"dev": to}, device_id_type=MESH,
        )

    near_first(lambda to: id_copy(ids_out.at[to], ids_in.at[me], to, my_chunk).start())
    copies[0].wait()
    pool_turn(tables_ref, turned_ref)
    for copy in copies[1:] + small_copies[3:]:
        copy.wait()

    def ids_of(group, count):
        some = pl.ds(0, count)
        return id_copy(ids_out.at[some], ids_in.at[some], (me + 1) % n, group)

    def row_copy(src, dst, to, chunk):
        return pltpu.make_async_remote_copy(
            src_ref=src, dst_ref=dst, send_sem=send_sem.at[0], recv_sem=recv_sems.at[chunk],
            device_id={"dev": to}, device_id_type=MESH,
        )

    def block(ref, device):
        return ref.at[pl.ds(pl.multiple_of(device * ROOM, ROOM), ROOM), :]

    def wait_ids(chunk):
        @pl.when(chunk == my_chunk)
        def _():
            ids_of(chunk, 3).wait_recv()

        @pl.when(chunk != my_chunk)
        def _():
            ids_of(chunk, 4).wait_recv()

    def step(t, carry):
        chunks = [target(t, half) for half in range(2)]
        for half in range(2):
            wait_ids(chunks[half])
            ids_wide[half * 4 : half * 4 + 4] = ids_in[
                pl.ds(pl.multiple_of(chunks[half] * 4, 4), 4)
            ].astype(I32)
        pool_setup(
            lambda q, j: ids_wide[pl.ds(q, 2, stride=4), j, :], y_ref, code_ref, pos_ref, scale_ref
        )
        for j in range(4):
            pool_table(j, turned_ref, y_ref, code_ref, scale_ref, xt_ref)
        blocks = pool_pack(pos_ref, xt_ref)
        for half in range(2):
            send_ref[pl.ds(pl.multiple_of(chunks[half] * 4 * ROOM, 4 * ROOM), 4 * ROOM), :] = blocks[half]
        for u in range(2):
            weight_cut(2 * t + u, raw_ref, plane_ref)

        for i in range(4):
            for half in range(2):
                to = chunks[half] * 4 + ((my_place + i) & 3)

                @pl.when(to != me)
                def _():
                    row_copy(block(send_ref, to), block(recv_ref, me), to, my_chunk).start()

        return carry

    lax.fori_loop(0, GROUPS, step, 0)
    target_setup(inverse_ref, counts_ref, order_ref, compress_ref, turn_ref, mix_ref)
    perm_ref[...] = order_columns(order_ref).astype(F32).T.astype(BF)
    for c in range(2 * GROUPS):
        cols_ref[c] = mix_ref[:, c * 16 : c * 16 + 16]

    def clear(w, carry):
        rows = pl.ds(pl.multiple_of(arrived(GROUPS - 4 + w // 2, w % 2) * 16, 16), 16)
        feat_ref[:, :, rows, :] = jnp.zeros((64, 2, 16, 128), BF)
        return carry

    lax.fori_loop(0, 8, clear, 0)
    mine = pl.ds(pl.multiple_of(me * ROOM, ROOM), ROOM)
    recv_ref[mine, :] = send_ref[mine, :]

    def take(u, v):
        chunk = arrived(u, v)

        @pl.when(chunk == my_chunk)
        def _():
            rows = pl.ds(0, 3 * ROOM)
            row_copy(send_ref.at[rows, :], recv_ref.at[rows, :], (me + 1) % n, chunk).wait_recv()

        @pl.when(chunk != my_chunk)
        def _():
            rows = pl.ds(0, 4 * ROOM)
            row_copy(send_ref.at[rows, :], recv_ref.at[rows, :], (me + 1) % n, chunk).wait_recv()

        pick_chunk(chunk, recv_ref, turn_ref, feat_ref)

    def turn_and_take(w, carry):
        weight_plane(w, perm_ref, plane_ref, raw_ref)
        take(w // 2, w % 2)
        return carry

    def only_take(w, carry):
        take(w // 2, w % 2)
        return carry

    lax.fori_loop(0, 16, turn_and_take, 0)
    lax.fori_loop(16, 2 * GROUPS - 8, only_take, 0)

    def keep(i, value):
        sum_ref[i] = value

    mixing(mix_ref[...], lambda i, v: feat_ref[i, v], keep)
    lax.fori_loop(2 * GROUPS - 8, 2 * GROUPS, only_take, 0)
    last = [arrived(GROUPS - 4 + w // 2, w % 2) for w in range(8)]
    zero = jnp.zeros((16, 128), BF)

    def settle(i, value):
        mixed = (sum_ref[i] + value).astype(BF)
        for v in range(2):
            left_ref[i, v, v * 16 : v * 16 + 16, :] = mixed[:, v * 128 : v * 128 + 128]
            left_ref[i, v, 16 - v * 16 : 32 - v * 16, :] = zero

    mixing(
        jnp.concatenate([cols_ref[c] for c in last], axis=1),
        lambda i, v: jnp.concatenate(
            [feat_ref[i, v, pl.ds(pl.multiple_of(c * 16, 16), 16), :] for c in last], axis=0
        ),
        settle,
    )
    finish(
        feat_ref, lambda k, at: raw_ref[at, pl.ds(pl.multiple_of(k * 512, 512), 512), :],
        bias_ref, out_ref, left_ref, pair_ref, acc_ref,
    )
    ids_of(my_chunk, n - 1).wait_send()
    rows = pl.ds(0, (n - 1) * ROOM)
    row_copy(send_ref.at[rows, :], recv_ref.at[rows, :], (me + 1) % n, my_chunk).wait_send()


def shards(tables, bag_rows, bag_lengths, row_counts, inverse, table_order, compress, top_weight, top_bias):
    order = table_order.reshape(1, -1)
    bias = top_bias.reshape(1, -1)
    rows = bag_rows[0].transpose(1, 2, 0)
    lens = bag_lengths[0].transpose(1, 0)
    samples, units = inverse.shape[0], top_weight.shape[1]
    anywhere = pl.BlockSpec(memory_space=pl.ANY)
    scratch = (
        [pltpu.VMEM(x.shape, x.dtype) for x in (rows, lens, row_counts, inverse, order, compress, bias)]
        + [pltpu.VMEM(tables.shape, BF)]
        + pool_scratch()
        + [
            pltpu.VMEM((units // 128, top_weight.shape[0], 128), BF),
            pltpu.VMEM((16, units // 128, 512, 128), BF),
            pltpu.VMEM((512, 512), BF),
            pltpu.VMEM((128, 4, 128), jnp.int16),
            pltpu.VMEM((128, 4, 128), jnp.int16),
            pltpu.VMEM((16, 4, 128), I32),
            pltpu.VMEM((128 * ROOM, 128), BF),
            pltpu.VMEM((128 * ROOM, 128), BF),
        ]
        + score_scratch()
        + [pltpu.VMEM((2 * GROUPS, 16, 16), BF)]
        + [
            pltpu.SemaphoreType.DMA((12,)),
            pltpu.SemaphoreType.DMA((2 * GROUPS,)),
            pltpu.SemaphoreType.DMA((2,)),
            pltpu.SemaphoreType.DMA((2 * GROUPS,)),
        ]
    )
    hidden = pl.pallas_call(
        lookup_body,
        out_shape=jax.ShapeDtypeStruct((samples, units), F32),
        in_specs=[anywhere] * 9,
        out_specs=VM,
        scratch_shapes=scratch,
        compiler_params=pltpu.CompilerParams(vmem_limit_bytes=BIG, collective_id=0, has_side_effects=True),
        cost_estimate=pl.CostEstimate(flops=3 * 10**10, bytes_accessed=16 << 20, transcendentals=0),
    )(rows, lens, row_counts, inverse, order, compress, bias, tables, top_weight)
    return jnp.maximum(hidden, 0.0).astype(BF)


def solution(mesh):
    return jax.shard_map(
        shards,
        mesh=mesh,
        in_specs=(
            P("dev", None, None),
            P(("rep", "dev"), None, None, None),
            P(("rep", "dev"), None, None),
            P(("rep", "dev"), None),
            P(("rep", "dev"), None),
            P(),
            P(),
            P(),
            P(),
        ),
        out_specs=P(("rep", "dev"), None),
        check_vma=False,
    )
```
